32 devices in a mesh: dp: 8 (over z, y), mp: 4 (over x, core).
Axes of the slice: x: 2, y: 2, z: 4, core: 2. Of those that a mesh axis runs over, the one named last changes fastest.
Arguments:
- tokens: bfloat16 [8, 1024, 1280], P('dp', 'mp'), may hold values from -6 to 6
- sizes: float32 [8, 1024], P('dp'), may hold values from 1 to 8
- ln1_gain: float32 [1280], replicated, may hold values from 0.25 to 1.75
- qkv_weight: bfloat16 [3, 1280, 1280], P(None, 'dp', 'mp'), may hold values from -0.15625 to 0.15625
- proj_weight: bfloat16 [1280, 1280], P('mp', 'dp'), may hold values from -0.15625 to 0.15625
- ln2_gain: float32 [1280], replicated, may hold values from 0.25 to 1.75
- fc1_weight: bfloat16 [1280, 5120], P('dp', 'mp'), may hold values from -0.15625 to 0.15625
- fc1_bias: float32 [5120], P('mp'), may hold values from -3 to 3
- fc2_weight: bfloat16 [5120, 1280], P('mp', 'dp'), may hold values from -0.078125 to 0.078125
- pair_source: int32 [8, 16], P('dp'), may hold values from 0 to 1022, as said below
- pair_target: int32 [8, 16], P('dp'), may hold values from 1 to 1023, as said below
- kept_order: int32 [8, 1008], P('dp'), may hold values from 0 to 1023, as said below
Outputs:
- merged_out: bfloat16 [8, 1008, 1280], P('dp', 'mp')
The draws below stay inside these ranges and needn't reach their ends.
Inputs may be any that keep to these rules, and one draw needn't show every extreme that they name: `pair_source`: in each image the 16 entries are distinct even token indices. `pair_target`: odd token indices; several sources may join the same target. `kept_order`: in each image every token index that is not in pair_source appears exactly once.
All inputs are finite; a program needn't handle non-finite values.
Results may differ from the reference program's by a relative error of at most 0.017.
Values may be sent and summed in bfloat16 or wider, within the bound.
A program may use at most 64 MiB of HBM per device.

```python
import math
import jax
import jax.numpy as jnp
from jax import lax

D = 1280
HEADS = 16
FF = 5120
N = 1024
R = 16
IMAGES = 8


def merge_plan(key):
    image_keys = jax.random.split(jax.random.fold_in(key, 7), IMAGES)

    def one_plan(image_key):
        first, second, third = jax.random.split(image_key, 3)
        shuffled = jax.random.permutation(first, N // 2).astype(jnp.int32)
        sources = 2 * shuffled[:R]
        targets = 2 * jax.random.randint(second, (R,), 0, N // 2).astype(jnp.int32) + 1
        kept_even = 2 * shuffled[R:]
        odd_tokens = 2 * jnp.arange(N // 2, dtype=jnp.int32) + 1
        remaining = jnp.concatenate([kept_even, odd_tokens])
        ordered = jax.random.permutation(third, remaining).astype(jnp.int32)
        return (sources, targets, ordered)
    return jax.vmap(one_plan)(image_keys)


def draw_pair_source(key, part):
    return merge_plan(key)[0]


def draw_pair_target(key, part):
    return merge_plan(key)[1]


def draw_kept_order(key, part):
    return merge_plan(key)[2]


def shard_levels(own_key, shape, cuts, low, high):
    def one(dim, blocks):
        heights = jax.random.uniform(jax.random.fold_in(jax.random.fold_in(own_key, 6), dim), (blocks,), jnp.float32, low / len(cuts), high / len(cuts))
        return jnp.repeat(jnp.exp(heights), shape[dim] // blocks).reshape((-1,) + (1,) * (len(shape) - dim - 1))

    factor_of = one(*cuts[0])
    for cut in cuts[1:]:
        factor_of = factor_of * one(*cut)
    return factor_of


def centred(key, extent, deviation, most, cuts=(), kind=jnp.bfloat16):
    values = deviation * jax.random.normal(key, extent, jnp.float32)
    if cuts:
        values = values * shard_levels(key, extent, cuts, -0.22, 0.18)
    return jnp.clip(values, -most, most).astype(kind)


def setup_inputs(seed: int = 0) -> dict:
    streams_of = jax.random.split(jax.random.key(seed), 13)
    return {
        "tokens": centred(streams_of[0], (IMAGES, N, D), 1.0, 6.0, ((0, 8), (1, 4))),
        "sizes": jnp.clip(jnp.exp(math.log(8.0) - 2.0794415 * jax.random.uniform(streams_of[1], (IMAGES, N), jnp.float32) ** shard_levels(streams_of[1], (IMAGES, N), ((0, 8),), -0.2, 0.2)), 1.0, 8.0),
        "ln1_gain": jnp.clip(1.0 + 0.15 * jax.random.normal(streams_of[2], (D,), jnp.float32), 0.25, 1.75),
        "qkv_weight": centred(streams_of[3], (3, D, D), D ** -0.5, 0.15625, ((1, 8), (2, 4))),
        "proj_weight": centred(streams_of[4], (D, D), D ** -0.5, 0.15625, ((0, 4), (1, 8))),
        "ln2_gain": jnp.clip(1.0 + 0.15 * jax.random.normal(streams_of[5], (D,), jnp.float32), 0.25, 1.75),
        "fc1_weight": centred(streams_of[6], (D, FF), D ** -0.5, 0.15625, ((0, 8), (1, 4))),
        "fc1_bias": centred(streams_of[7], (FF,), 0.5, 3.0, ((0, 4),), jnp.float32),
        "fc2_weight": centred(streams_of[8], (FF, D), FF ** -0.5, 0.078125, ((0, 4), (1, 8))),
        "pair_source": draw_pair_source(jax.random.fold_in(streams_of[12], 71), 0),
        "pair_target": draw_pair_target(jax.random.fold_in(streams_of[12], 71), 0),
        "kept_order": draw_kept_order(jax.random.fold_in(streams_of[12], 71), 0),
    }


def layer_norm(values, gain):
    center = values - lax.optimization_barrier(jnp.mean(values, axis=-1, keepdims=True))
    spread = lax.optimization_barrier(jnp.mean(center * center, axis=-1, keepdims=True))
    return center * lax.rsqrt(spread + 1e-06) * gain

def one_image(tokens, sizes, source_ids, target_ids, order, ln1_gain, qkv_weight, proj_weight, ln2_gain, fc1_weight, fc1_bias, fc2_weight):
    width = tokens.shape[1]
    head_size = width // HEADS
    base = tokens.astype(jnp.float32)
    normed = layer_norm(base, ln1_gain).astype(jnp.bfloat16)
    query = jnp.dot(normed, qkv_weight[0], preferred_element_type=jnp.float32).astype(jnp.bfloat16)
    keys = jnp.dot(normed, qkv_weight[1], preferred_element_type=jnp.float32).astype(jnp.bfloat16)
    values = jnp.dot(normed, qkv_weight[2], preferred_element_type=jnp.float32).astype(jnp.bfloat16)
    length = tokens.shape[0]
    query = query.reshape(length, HEADS, head_size).astype(jnp.float32)
    keys = keys.reshape(length, HEADS, head_size).astype(jnp.float32)
    values = values.reshape(length, HEADS, head_size).astype(jnp.float32)
    scores = jnp.einsum('qhe,khe->hqk', query, keys) / math.sqrt(head_size) + jnp.log(sizes)[None, None, :]
    weights = jax.nn.softmax(scores, axis=-1).astype(jnp.bfloat16)
    attended = jnp.einsum('hqk,khe->qhe', weights.astype(jnp.float32), values).astype(jnp.bfloat16)
    attended = attended.reshape(length, width)
    residual = base + jnp.dot(attended, proj_weight, preferred_element_type=jnp.float32)
    positions = jnp.arange(length, dtype=jnp.int32)
    hits = (positions[None, :] == source_ids[:, None]).astype(jnp.int32)
    destination = positions + lax.optimization_barrier(jnp.sum(hits * (target_ids[:, None] - positions[None, :]), axis=0))
    table = (order[:, None] == destination[None, :]).astype(jnp.float32)
    numerator = jnp.dot(table, sizes[:, None] * residual, precision=lax.Precision.HIGHEST)
    merged_size = jnp.dot(table, sizes, precision=lax.Precision.HIGHEST)
    merged = numerator / merged_size[:, None]
    normed_two = layer_norm(merged, ln2_gain).astype(jnp.bfloat16)
    hidden = jax.nn.gelu(jnp.dot(normed_two, fc1_weight, preferred_element_type=jnp.float32) + fc1_bias).astype(jnp.bfloat16)
    return (merged + jnp.dot(hidden, fc2_weight, preferred_element_type=jnp.float32)).astype(jnp.bfloat16)

def reference(tokens, sizes, ln1_gain, qkv_weight, proj_weight, ln2_gain, fc1_weight, fc1_bias, fc2_weight, pair_source, pair_target, kept_order):

    def apply(item):
        return one_image(item[0], item[1], item[2], item[3], item[4], ln1_gain, qkv_weight, proj_weight, ln2_gain, fc1_weight, fc1_bias, fc2_weight)
    return lax.map(apply, (tokens, sizes, pair_source, pair_target, kept_order))
```

```python
import functools
import math

import jax
import jax.numpy as jnp
from jax import lax
from jax.experimental import pallas as pl
from jax.experimental.pallas import tpu as pltpu
from jax.sharding import PartitionSpec as P

HEADS = 16


def layer_norm(values, gain):
    center = values - jnp.mean(values, axis=-1, keepdims=True)
    spread = jnp.mean(center * center, axis=-1, keepdims=True)
    return center * lax.rsqrt(spread + 1e-06) * gain


def powers(count):
    bits = []
    bit = 1
    while bit < count:
        bits.append(bit)
        bit *= 2
    return bits


def toggled(index, mask):
    for bit in powers(mask + 1):
        if mask & bit:
            index = index + bit * (1 - 2 * lax.rem(lax.div(index, bit), 2))
    return index


def greet(peers):
    barrier = pltpu.get_barrier_semaphore()
    for axis, peer in peers:
        pl.semaphore_signal(
            barrier, inc=1, device_id={axis: peer}, device_id_type=pl.DeviceIdType.MESH
        )
    pl.semaphore_wait(barrier, len(peers))


class Copies:
    def __init__(self, send, recv):
        self.send, self.recv, self.made = send, recv, []

    def start(self, source, target, axis, peer):
        number = len(self.made)
        copy = pltpu.make_async_remote_copy(
            src_ref=source,
            dst_ref=target,
            send_sem=self.send.at[number],
            recv_sem=self.recv.at[number],
            device_id={axis: peer},
            device_id_type=pl.DeviceIdType.MESH,
        )
        copy.start()
        self.made.append(copy)
        return copy


def rows_of(out, owner, rows):
    span = pl.ds(pl.multiple_of(owner * rows, 16), rows)
    if len(out.shape) == 3:
        return out.at[:, span, :]
    return out.at[span, :]


class Waits:
    def __init__(self):
        self.seen = set()

    def ready(self, copy):
        if id(copy) not in self.seen:
            copy.wait_recv()
            self.seen.add(id(copy))


def dp_peers(dp):
    me = lax.axis_index("dp")
    return me, toggled(me, 1), lax.rem(me + 2, dp), lax.rem(me + dp - 2, dp)


def start_dp(own, out, copies, dp):
    me, pair, after, before = dp_peers(dp)
    here = rows_of(out, me, own.shape[-2])
    return [copies.start(own, here, "dp", peer) for peer in (pair, after, before)]


def relay_dp(own, out, copies, waits, state, dp, step):
    me, pair, after, before = dp_peers(dp)
    ring = dp // 2
    rows = own.shape[-2]
    other, forward, backward = state
    block = rows_of(out, lax.rem(me - 2 * step + 2 * dp, dp), rows)
    waits.ready(forward)
    if step < ring // 2:
        state[1] = copies.start(block, block, "dp", after)
    copies.start(block, block, "dp", pair)
    if step < ring - step:
        block = rows_of(out, toggled(lax.rem(me + 2 * (step - 1), dp), 1), rows)
        waits.ready(other)
        state[0] = copies.start(block, block, "dp", before)
        if step + 1 < ring - step - 1:
            block = rows_of(out, lax.rem(me + 2 * step, dp), rows)
            waits.ready(backward)
            state[2] = copies.start(block, block, "dp", before)


def gather_kernel(dp, mp, *refs):
    own, out = refs[:2], refs[2:4]
    send, recv, local = refs[4:]
    at = lax.axis_index("mp")
    me, pair, after, before = dp_peers(dp)
    greet(
        [("mp", toggled(at, bit)) for bit in powers(mp)]
        + [("dp", pair), ("dp", after), ("dp", before)]
    )
    copies, waits = Copies(send, recv), Waits()
    heads = start_dp(own[1], out[1], copies, dp)
    mine = rows_of(out[0], at, own[0].shape[0])
    bits = list(reversed(powers(mp)))
    here = {bit: copies.start(own[0], mine, "mp", toggled(at, bit)) for bit in bits}
    stays = []
    for number, owner in ((0, at), (1, me)):
        keep = pltpu.make_async_copy(
            own[number], rows_of(out[number], owner, own[number].shape[-2]), local.at[number]
        )
        keep.start()
        stays.append(keep)
    relay_dp(own[1], out[1], copies, waits, heads, dp, 1)
    held = [0]
    for bit in bits:
        for k in list(held):
            if k:
                waits.ready(here[k])
                block = rows_of(out[0], toggled(at, k), own[0].shape[0])
                here[k ^ bit] = copies.start(block, block, "mp", toggled(at, bit))
            held.append(k ^ bit)
    for step in range(2, dp // 4 + 1):
        relay_dp(own[1], out[1], copies, waits, heads, dp, step)
    for copy in copies.made:
        waits.ready(copy)
        copy.wait_send()
    for keep in stays:
        keep.wait()


def gather_all(normed, heads):
    dp, mp = lax.axis_size("dp"), lax.axis_size("mp")
    total = (mp - 1) + (dp - 1)
    shapes = [
        (mp * normed.shape[0], normed.shape[1]),
        (dp * heads.shape[0], heads.shape[1]),
    ]
    return pl.pallas_call(
        functools.partial(gather_kernel, dp, mp),
        out_shape=[jax.ShapeDtypeStruct(shape, jnp.bfloat16) for shape in shapes],
        in_specs=[pl.BlockSpec(memory_space=pltpu.VMEM)] * 2,
        out_specs=[pl.BlockSpec(memory_space=pl.ANY)] * 2,
        scratch_shapes=[
            pltpu.SemaphoreType.DMA((total,)),
            pltpu.SemaphoreType.DMA((total,)),
            pltpu.SemaphoreType.DMA((2,)),
        ],
        compiler_params=pltpu.CompilerParams(collective_id=0, has_side_effects=True),
        cost_estimate=pl.CostEstimate(
            flops=10**10, bytes_accessed=10**8, transcendentals=0
        ),
        name="gather_all",
    )(normed, heads)


def reduce_kernel(dp, mp, last, *refs):
    if last:
        parts, extra, out, held, landing, send, recv = refs
    else:
        parts, extra, own, out, whole, weight, held, landing, normed, send, recv, local = refs
    at = lax.axis_index("mp")
    peers = [("mp", toggled(at, bit)) for bit in powers(mp)]
    if not last:
        peers += [("dp", peer) for peer in dp_peers(dp)[1:]]
    greet(peers)
    copies, waits = Copies(send, recv), Waits()
    slots = 0
    stored = {k: None for k in range(mp)}
    if not last:
        state = start_dp(own, weight, copies, dp)
        rest = pltpu.make_async_copy(
            own, rows_of(weight, lax.axis_index("dp"), own.shape[0]), local.at[1]
        )
        rest.start()

    def source(k):
        return parts.at[toggled(at, k)] if stored[k] is None else held.at[k]

    for bit in powers(mp):
        moving = [k for k in reversed(range(mp)) if k in stored and k & bit]
        flights = []
        for k in moving:
            flights.append(
                (k, slots, copies.start(source(k), landing.at[slots], "mp", toggled(at, bit)))
            )
            slots += 1
        for k, slot, copy in flights:
            waits.ready(copy)
            kept = k ^ bit
            total = source(kept)[...].astype(jnp.float32) + landing[slot].astype(jnp.float32)
            if 2 * bit < mp:
                held[kept] = total.astype(jnp.bfloat16)
                stored[kept] = True
            del stored[k]
        if not last and bit == 1:
            relay_dp(own, weight, copies, waits, state, dp, 1)
    if last:
        out[...] = (extra[...] + total).astype(out.dtype)
    else:
        out[...] = total
        normed[...] = layer_norm(total, extra[...]).astype(jnp.bfloat16)
        keep = pltpu.make_async_copy(normed, whole.at[at], local.at[0])
        keep.start()
        bits = list(reversed(powers(mp)))
        here = {
            bit: copies.start(normed, whole.at[at], "mp", toggled(at, bit)) for bit in bits
        }
        for step in range(2, dp // 4 + 1):
            relay_dp(own, weight, copies, waits, state, dp, step)
        near = [0]
        for bit in bits:
            for k in list(near):
                if k:
                    waits.ready(here[k])
                    block = whole.at[toggled(at, k)]
                    here[k ^ bit] = copies.start(block, block, "mp", toggled(at, bit))
                near.append(k ^ bit)
        keep.wait()
        rest.wait()
    for copy in copies.made:
        waits.ready(copy)
        copy.wait_send()


def reduce_parts(parts, extra, own=None):
    mp, rows, width = parts.shape
    dp = lax.axis_size("dp")
    last = own is None
    operands = [parts, extra] if last else [parts, extra, own]
    vmem = pl.BlockSpec(memory_space=pltpu.VMEM)
    out_shape = [
        jax.ShapeDtypeStruct((rows, width), jnp.bfloat16 if last else jnp.float32)
    ]
    out_specs = [vmem]
    scratch = [
        pltpu.VMEM((mp, rows, width), jnp.bfloat16),
        pltpu.VMEM((mp - 1, rows, width), jnp.bfloat16),
    ]
    total = mp - 1
    if not last:
        out_shape.append(jax.ShapeDtypeStruct((mp, rows, width), jnp.bfloat16))
        out_shape.append(jax.ShapeDtypeStruct((dp * own.shape[0], own.shape[1]), jnp.bfloat16))
        out_specs += [pl.BlockSpec(memory_space=pl.ANY)] * 2
        scratch.append(pltpu.VMEM((rows, width), jnp.bfloat16))
        total = 2 * total + dp - 1
    scratch += [pltpu.SemaphoreType.DMA((total,)), pltpu.SemaphoreType.DMA((total,))]
    if not last:
        scratch.append(pltpu.SemaphoreType.DMA((2,)))
    return pl.pallas_call(
        functools.partial(reduce_kernel, dp, mp, last),
        out_shape=out_shape,
        in_specs=[vmem] * len(operands),
        out_specs=out_specs,
        scratch_shapes=scratch,
        compiler_params=pltpu.CompilerParams(
            collective_id=2 if last else 1, has_side_effects=True
        ),
        cost_estimate=pl.CostEstimate(
            flops=10**10, bytes_accessed=10**8, transcendentals=0
        ),
        name="reduce_last" if last else "reduce_norm_gather",
    )(*operands)


def shards(
    tokens,
    sizes,
    ln1_gain,
    qkv_weight,
    proj_weight,
    ln2_gain,
    fc1_weight,
    fc1_bias,
    fc2_weight,
    pair_source,
    pair_target,
    kept_order,
):
    images, own_tokens, width = tokens.shape
    length = sizes.shape[1]
    kept_total = kept_order.shape[1]
    count = lax.axis_size("mp")
    me = lax.axis_index("mp")
    kept_own = kept_total // count
    padded = -(-kept_own // 16) * 16
    head_size = width // HEADS
    local_width = qkv_weight.shape[2]
    local_heads = local_width // head_size

    base = tokens.astype(jnp.float32)
    normed = layer_norm(base, ln1_gain).astype(jnp.bfloat16)
    whole, heads_whole = gather_all(
        normed.reshape(own_tokens, width),
        jnp.concatenate(
            [qkv_weight[0], qkv_weight[1], qkv_weight[2], proj_weight.T], axis=1
        ),
    )
    whole = whole[None]
    whole, heads_whole, late = lax.optimization_barrier((whole, heads_whole, fc1_weight))
    fc1 = lax.all_gather(late, "dp", axis=0, tiled=True)

    positions = jnp.arange(length, dtype=jnp.int32)
    order = jnp.pad(
        kept_order.reshape(images, count, kept_own),
        ((0, 0), (0, 0), (0, padded - kept_own)),
        constant_values=-1,
    ).reshape(images, count * padded)
    hits = positions[None, None, :] == pair_source[:, :, None]
    destination = positions[None, :] + jnp.sum(
        jnp.where(hits, pair_target[:, :, None] - positions[None, None, :], 0), axis=1
    )
    joins = order[:, :, None] == destination[:, None, :]
    shares = jnp.where(joins, sizes[:, None, :], 0.0)
    merged_size = jnp.sum(shares, axis=2, keepdims=True)
    shares = (shares / jnp.where(merged_size > 0, merged_size, 1.0)).astype(jnp.bfloat16)
    own_shares = lax.dynamic_slice_in_dim(shares, me * own_tokens, own_tokens, 2)

    projected = jnp.einsum(
        "ind,df->inf", whole, heads_whole[:, : 3 * local_width], preferred_element_type=jnp.float32
    ).astype(jnp.bfloat16)
    shaped = [
        projected[:, :, c * local_width : (c + 1) * local_width].reshape(
            images, length, local_heads, head_size
        )
        for c in range(3)
    ]
    size_bias = jnp.log(sizes)[:, None, None, :]
    block = min(512, length)
    outputs = []
    for begin in range(0, length, block):
        scores = (
            jnp.einsum(
                "iqhe,ikhe->ihqk",
                shaped[0][:, begin : begin + block],
                shaped[1],
                preferred_element_type=jnp.float32,
            )
            / math.sqrt(head_size)
            + size_bias
        )
        weights = jax.nn.softmax(scores, axis=-1).astype(jnp.bfloat16)
        outputs.append(
            jnp.einsum("ihqk,ikhe->iqhe", weights, shaped[2], preferred_element_type=jnp.float32)
            .astype(jnp.bfloat16)
            .reshape(images, block, local_width)
        )
    attended = jnp.concatenate(outputs, axis=1)

    joined = jnp.einsum(
        "ijn,ind->ijd", shares, attended, preferred_element_type=jnp.float32
    ).astype(jnp.bfloat16)

    left, right = lax.optimization_barrier(
        (
            jnp.concatenate([joined, own_shares], axis=2),
            jnp.concatenate([heads_whole[:, 3 * local_width :].T, tokens[0]], axis=0),
        )
    )
    parts = jnp.einsum("ijd,de->ije", left, right, preferred_element_type=jnp.float32)
    parts = parts.astype(jnp.bfloat16).reshape(count, padded, width)
    merged, gathered, fc2 = reduce_parts(parts, ln2_gain.reshape(1, width), fc2_weight.T)
    hidden_sum = jnp.einsum(
        "md,df->mf", gathered.reshape(count * padded, width), fc1,
        preferred_element_type=jnp.float32,
    )
    hidden = jax.nn.gelu(hidden_sum + fc1_bias).astype(jnp.bfloat16)
    partial_out = jnp.einsum("mf,df->md", hidden, fc2, preferred_element_type=jnp.float32)
    partial_out = partial_out.astype(jnp.bfloat16).reshape(count, padded, width)
    out = reduce_parts(partial_out, merged)[0]
    return out[None, :kept_own]


LOG2E = math.log2(math.e)
KINDS = ("E1", "E2", "Y4", "N1", "N2", "M1", "M2", "M3", "M4", "Y1", "Y2", "Y3")
ARRAYS = ("k", "v", "q", "p", "f1a", "f1b", "f2a", "f2b")


def nt_dot(left, right):
    return lax.dot_general(
        left, right, (((1,), (1,)), ((), ())), preferred_element_type=jnp.float32
    )


class Streams:
    def __init__(self, dp, homes, send, recv, local):
        me = lax.axis_index("dp")
        z, y = lax.div(me, 2), lax.rem(me, 2)
        high = lax.div(z, 2)
        step = 1 - 2 * high
        self.end = lax.rem(lax.div(z + 1, 2), 2) == 0
        self.mid = lax.rem(lax.div(z + 1, 2), 2) == 1
        self.me = me
        self.pair = z * 2 + 1 - y
        self.inner = (z + step) * 2 + y
        self.outer = lax.rem((z - step) * 2 + y + dp, dp)
        self.ahead = [lax.rem((z + step * k) * 2 + y + dp, dp) for k in range(4)]
        self.homes, self.send, self.recv, self.local = homes, send, recv, local
        self.peers = {"inner": self.inner, "outer": self.outer, "pair": self.pair}

    def block(self, name, owner, part=None):
        source, target, rows = self.homes[name]
        low, count = 0, rows
        if part is not None:
            low, count = part * (rows // 2), rows // 2
        return target(pl.ds(pl.multiple_of(owner * rows + low, 16), count))

    def own(self, name):
        return self.homes[name][0]

    def copy(self, name, kind, source, target, peer):
        number = ARRAYS.index(name) * len(KINDS) + KINDS.index(kind)
        return pltpu.make_async_remote_copy(
            src_ref=source,
            dst_ref=target,
            send_sem=self.send.at[number],
            recv_sem=self.recv.at[number],
            device_id={"dp": self.peers[peer]},
            device_id_type=pl.DeviceIdType.MESH,
        )

    def move(self, name, kind, owner, peer, part=None):
        block = self.block(name, owner, part)
        self.copy(name, kind, block, block, peer).start()

    def arrived(self, name, *kinds):
        for kind in kinds:
            block = self.block(name, self.me, 0 if kind in ("Y4", "M4") else None)
            self.copy(name, kind, block, block, "pair").wait_recv()

    def stay(self, name):
        return pltpu.make_async_copy(
            self.own(name), self.block(name, self.me), self.local.at[ARRAYS.index(name)]
        )

    def s0(self, name):
        here = self.block(name, self.me)

        @pl.when(self.end)
        def _():
            self.copy(name, "E1", self.own(name), here, "inner").start()

        @pl.when(self.mid)
        def _():
            self.copy(name, "M1", self.own(name), here, "outer").start()
            self.copy(name, "N1", self.own(name), here, "inner").start()

        self.copy(name, "Y1", self.own(name), here, "pair").start()
        self.stay(name).start()

    def s1(self, name):
        @pl.when(self.end)
        def _():
            self.arrived(name, "M1")
            self.move(name, "Y4", self.ahead[1], "pair", 0)
            self.arrived(name, "Y1")
            self.move(name, "E2", self.pair, "inner")

        @pl.when(self.mid)
        def _():
            self.arrived(name, "N1")
            self.move(name, "M2", self.ahead[1], "outer")
            self.move(name, "Y2", self.ahead[1], "pair")
            self.arrived(name, "E1")
            self.move(name, "N2", self.outer, "inner")
            self.arrived(name, "Y1")
            self.move(name, "M4", self.pair, "outer", 1)

    def s2(self, name):
        @pl.when(self.end)
        def _():
            self.arrived(name, "M2")
            self.move(name, "Y2", self.ahead[2], "pair")

        @pl.when(self.mid)
        def _():
            self.arrived(name, "N2")
            self.move(name, "M3", self.ahead[2], "outer")
            self.move(name, "Y3", self.ahead[2], "pair")

    def s3(self, name):
        @pl.when(self.end)
        def _():
            self.arrived(name, "M3")
            self.move(name, "Y3", self.ahead[3], "pair")

    def near(self, name):
        self.stay(name).wait()

        @pl.when(self.end)
        def _():
            self.arrived(name, "M4", "Y4")

        @pl.when(self.mid)
        def _():
            self.arrived(name, "E2")

    def far(self, name):
        self.arrived(name, "Y2", "Y3")

    def full(self, name):
        self.near(name)
        self.far(name)

    def sent(self, name):
        def drain(*kinds):
            for kind in kinds:
                block = self.block(name, self.me, 0 if kind in ("Y4", "M4") else None)
                self.copy(name, kind, block, block, "pair").wait_send()

        drain("Y1", "Y2", "Y3")

        @pl.when(self.end)
        def _():
            drain("E1", "E2", "Y4")

        @pl.when(self.mid)
        def _():
            drain("N1", "N2", "M1", "M2", "M3", "M4")


def column_of(row, count):
    down = lax.broadcasted_iota(jnp.int32, (count, count), 0)
    over = lax.broadcasted_iota(jnp.int32, (count, count), 1)
    return jnp.sum(jnp.where(down == over, row, 0.0), axis=1, keepdims=True)


def layer_kernel(dp, mp, kept_own, *refs):
    (tokens, sizes, gain_one, qkv, proj, gain_two, fc1, bias, fc2, source, target, order) = refs[:12]
    out = refs[12]
    (tok, whole, wq, wp, w1, w2, shares, kbuf, qbuf, vbuf, attb, attended, parts, landing,
     merged, again, hidden, parts_two, landing_two, send, recv, local, msend, mrecv) = refs[13:]
    rows, width = tok.shape
    length = sizes.shape[1]
    local_width = wp.shape[1]
    local_heads, _, lanes = kbuf.shape
    head_size = local_width // local_heads
    half = width // 2
    at = lax.axis_index("mp")
    block_of = [toggled(at, k) for k in range(mp)]
    pair, across = block_of[1], block_of[2]

    cut = fc1.shape[1] // 2
    shard = fc1.shape[0]
    homes = {
        "k": (qkv.at[1], lambda r: wq.at[1, r, :], shard),
        "v": (qkv.at[2], lambda r: wq.at[2, r, :], shard),
        "q": (qkv.at[0], lambda r: wq.at[0, r, :], shard),
        "p": (proj, lambda r: wp.at[r, :], shard),
        "f1a": (fc1.at[:, pl.ds(0, cut)], lambda r: w1.at[r, pl.ds(0, cut)], shard),
        "f1b": (fc1.at[:, pl.ds(cut, cut)], lambda r: w1.at[r, pl.ds(cut, cut)], shard),
        "f2a": (fc2.at[:, pl.ds(0, cut)], lambda r: w2.at[r, pl.ds(0, cut)], shard),
        "f2b": (fc2.at[:, pl.ds(cut, cut)], lambda r: w2.at[r, pl.ds(cut, cut)], shard),
    }
    st = Streams(dp, homes, send, recv, local)

    load = pltpu.make_async_copy(tokens, tok, local.at[len(ARRAYS)])
    load.start()

    barrier = pltpu.get_barrier_semaphore()

    def hello(axis, peer):
        pl.semaphore_signal(
            barrier, inc=1, device_id={axis: peer}, device_id_type=pl.DeviceIdType.MESH
        )

    hello("mp", pair)
    hello("mp", across)
    hello("dp", st.pair)
    hello("dp", st.inner)

    @pl.when(st.mid)
    def _():
        hello("dp", st.outer)

    @pl.when(st.end)
    def _():
        pl.semaphore_wait(barrier, 4)

    @pl.when(st.mid)
    def _():
        pl.semaphore_wait(barrier, 5)

    st.s0("k")
    st.s0("v")

    made = []

    def give(src, dst, peer):
        copy = pltpu.make_async_remote_copy(
            src_ref=src,
            dst_ref=dst,
            send_sem=msend.at[len(made)],
            recv_sem=mrecv.at[len(made)],
            device_id={"mp": peer},
            device_id_type=pl.DeviceIdType.MESH,
        )
        copy.start()
        made.append(copy)
        return copy

    load.wait()
    slab = 32

    def norm_rows(i, carry):
        span = pl.ds(pl.multiple_of(i * slab, slab), slab)
        whole[at, span, :] = layer_norm(
            tok[span, :].astype(jnp.float32), gain_one[...]
        ).astype(jnp.bfloat16)
        return carry

    lax.fori_loop(0, rows // slab, norm_rows, 0)
    token_pair = give(whole.at[at], whole.at[at], pair)
    token_across = give(whole.at[at], whole.at[at], across)
    st.s0("q")

    position = lax.broadcasted_iota(jnp.int32, (1, length), 1).astype(jnp.float32)
    count = source.shape[1]
    source_column = column_of(source[...].astype(jnp.float32), count)
    target_column = column_of(target[...].astype(jnp.float32), count)
    destination = position + jnp.sum(
        jnp.where(position == source_column, target_column - position, 0.0),
        axis=0,
        keepdims=True,
    )
    size_row = sizes[...]
    order_row = order[...].astype(jnp.float32)

    def table(b, carry):
        shape = (rows, order.shape[1])
        down = lax.broadcasted_iota(jnp.int32, shape, 0)
        over = lax.broadcasted_iota(jnp.int32, shape, 1)
        mine = jnp.logical_and(over == down + b * kept_own, down < kept_own)
        wanted = jnp.sum(jnp.where(mine, order_row + 1.0, 0.0), axis=1, keepdims=True) - 1.0
        share = jnp.where(wanted == destination, size_row, 0.0)
        total = jnp.sum(share, axis=1, keepdims=True)
        share = share / jnp.where(total > 0, total, 1.0)
        shares[b] = share.astype(jnp.bfloat16)
        return carry

    lax.fori_loop(0, mp, table, 0)
    lane = lax.broadcasted_iota(jnp.int32, (length, lanes), 1)
    for h in range(local_heads):
        kbuf[h] = jnp.zeros((length, lanes), jnp.bfloat16)
        qbuf[h] = jnp.zeros((length, lanes), jnp.bfloat16)
        vbuf[h] = jnp.where(lane == head_size, 1.0, 0.0).astype(jnp.bfloat16)
    size_bias = jnp.log(size_row) * LOG2E

    st.s1("k")
    st.s0("p")
    st.s1("v")
    st.s2("k")
    st.s1("q")
    st.s2("v")
    st.s3("k")
    st.s1("p")
    st.s2("q")
    st.s3("v")
    token_across.wait_recv()
    token_far = give(whole.at[across], whole.at[across], pair)
    st.s0("f1a")
    st.s2("p")
    st.s3("q")
    st.s0("f1b")
    token_pair.wait_recv()
    token_far.wait_recv()

    def project(c, into, factor):
        def one(b, carry):
            product = jnp.dot(whole[b], wq[c], preferred_element_type=jnp.float32)
            if factor != 1.0:
                product = product * factor
            product = product.astype(jnp.bfloat16)
            span = pl.ds(pl.multiple_of(b * rows, rows), rows)
            for h in range(local_heads):
                into[h, span, 0:head_size] = product[:, h * head_size : (h + 1) * head_size]
            return carry

        lax.fori_loop(0, mp, one, 0)

    st.full("k")
    project(1, kbuf, 1.0)
    st.s3("p")
    st.full("v")
    project(2, vbuf, 1.0)
    st.full("q")
    project(0, qbuf, LOG2E / math.sqrt(head_size))

    duties = (
        (1, st.s1, "f1a"),
        (3, st.s1, "f1b"),
        (3, st.s0, "f2a"),
        (6, st.s2, "f1a"),
        (8, st.s2, "f1b"),
        (8, st.s0, "f2b"),
        (11, st.s3, "f1a"),
        (13, st.s3, "f1b"),
        (15, st.s1, "f2a"),
    )

    def attend(i, carry):
        for when, duty, name in duties:
            pl.when(i == when)(functools.partial(duty, name))
        b, h = lax.div(i, local_heads), lax.rem(i, local_heads)
        span = pl.ds(pl.multiple_of(b * rows, rows), rows)
        scores = nt_dot(qbuf[h, span, :], kbuf[h]) + size_bias
        top = jnp.max(scores, axis=1, keepdims=True)
        weights = jnp.exp2(scores - top).astype(jnp.bfloat16)
        mixed = jnp.dot(weights, vbuf[h], preferred_element_type=jnp.float32)
        attb[h, span, :] = (mixed / mixed[:, head_size : head_size + 1]).astype(jnp.bfloat16)
        return carry

    lax.fori_loop(0, mp * local_heads, attend, 0)
    for h in range(local_heads):
        attended[:, h * head_size : (h + 1) * head_size] = attb[h, :, 0:head_size]
    st.full("p")

    def part_of(block):
        share = shares[block]
        joined = jnp.dot(share, attended[...], preferred_element_type=jnp.float32)
        kept = shares[block, :, pl.ds(pl.multiple_of(at * rows, rows), rows)]
        return nt_dot(joined.astype(jnp.bfloat16), wp[...]) + jnp.dot(
            kept, tok[...], preferred_element_type=jnp.float32
        )

    parts[2] = part_of(block_of[3]).astype(jnp.bfloat16)
    first = give(parts.at[2], landing.at[2], pair)
    mine = part_of(across)
    first.wait_recv()
    parts[1] = (mine + landing[2].astype(jnp.float32)).astype(jnp.bfloat16)
    second = give(parts.at[1], landing.at[1], across)
    st.s1("f2b")
    parts[0] = part_of(pair).astype(jnp.bfloat16)
    third = give(parts.at[0], landing.at[0], pair)
    merged[...] = part_of(at)
    st.s2("f2a")
    third.wait_recv()
    second.wait_recv()
    st.s2("f2b")

    def norm_again(i, carry):
        span = pl.ds(pl.multiple_of(i * slab, slab), slab)
        total = (
            merged[span, :]
            + landing[0, span, :].astype(jnp.float32)
            + landing[1, span, :].astype(jnp.float32)
        )
        merged[span, :] = total
        again[at, span, :] = layer_norm(total, gain_two[...]).astype(jnp.bfloat16)
        return carry

    lax.fori_loop(0, rows // slab, norm_again, 0)
    norm_pair = give(again.at[at], again.at[at], pair)
    norm_across = give(again.at[at], again.at[at], across)
    st.s3("f2a")
    st.s3("f2b")
    st.full("f1a")
    st.full("f1b")

    def expand(block):
        product = jnp.dot(again[block], w1[...], preferred_element_type=jnp.float32)
        hidden[block] = jax.nn.gelu(product + bias[...]).astype(jnp.bfloat16)

    expand(at)
    norm_pair.wait_recv()
    expand(pair)
    norm_across.wait_recv()
    norm_far = give(again.at[across], again.at[across], pair)
    expand(across)
    norm_far.wait_recv()
    expand(block_of[3])

    near = lax.div(lax.div(st.me, 2), 2)

    def shrink(number, which):
        columns = pl.ds(pl.multiple_of(which * half, half), half)

        def piece(block):
            return nt_dot(hidden[block], w2[columns, :])

        parts_two[number, 2] = piece(block_of[3]).astype(jnp.bfloat16)
        one = give(parts_two.at[number, 2], landing_two.at[number, 2], pair)
        mine = piece(across)
        one.wait_recv()
        parts_two[number, 1] = (mine + landing_two[number, 2].astype(jnp.float32)).astype(
            jnp.bfloat16
        )
        two = give(parts_two.at[number, 1], landing_two.at[number, 1], across)
        parts_two[number, 0] = piece(pair).astype(jnp.bfloat16)
        three = give(parts_two.at[number, 0], landing_two.at[number, 0], pair)
        merged[:, columns] = merged[:, columns] + piece(at)
        return columns, two, three

    def finish(number, columns, two, three):
        three.wait_recv()
        two.wait_recv()
        out[:, columns] = (
            merged[:, columns]
            + landing_two[number, 0].astype(jnp.float32)
            + landing_two[number, 1].astype(jnp.float32)
        ).astype(out.dtype)

    st.near("f2a")
    st.near("f2b")
    close = shrink(0, near)
    st.far("f2a")
    st.far("f2b")
    distant = shrink(1, 1 - near)
    finish(0, *close)
    finish(1, *distant)
    for name in ARRAYS:
        st.sent(name)
    for copy in made:
        copy.wait_send()


def whole_layer(tokens, sizes, ln1_gain, qkv_weight, proj_weight, ln2_gain, fc1_weight, fc1_bias,
                fc2_weight, pair_source, pair_target, kept_order):
    dp, mp = lax.axis_size("dp"), lax.axis_size("mp")
    _, rows, width = tokens.shape
    length = sizes.shape[1]
    kept_own = kept_order.shape[1] // mp
    local_width = qkv_weight.shape[2]
    local_heads = HEADS * local_width // width
    head_size = local_width // local_heads
    lanes = -(-(head_size + 1) // 128) * 128
    hidden = fc1_weight.shape[1]
    bf16, f32 = jnp.bfloat16, jnp.float32
    vmem = pl.BlockSpec(memory_space=pltpu.VMEM)
    hbm = pl.BlockSpec(memory_space=pl.ANY)
    half = width // 2
    scratch = [
        pltpu.VMEM((rows, width), bf16),
        pltpu.VMEM((mp, rows, width), bf16),
        pltpu.VMEM((3, width, local_width), bf16),
        pltpu.VMEM((width, local_width), bf16),
        pltpu.VMEM((width, hidden), bf16),
        pltpu.VMEM((width, hidden), bf16),
        pltpu.VMEM((mp, rows, length), bf16),
        pltpu.VMEM((local_heads, length, lanes), bf16),
        pltpu.VMEM((local_heads, length, lanes), bf16),
        pltpu.VMEM((local_heads, length, lanes), bf16),
        pltpu.VMEM((local_heads, length, lanes), bf16),
        pltpu.VMEM((length, local_width), bf16),
        pltpu.VMEM((mp - 1, rows, width), bf16),
        pltpu.VMEM((mp - 1, rows, width), bf16),
        pltpu.VMEM((rows, width), f32),
        pltpu.VMEM((mp, rows, width), bf16),
        pltpu.VMEM((mp, rows, hidden), bf16),
        pltpu.VMEM((2, mp - 1, rows, half), bf16),
        pltpu.VMEM((2, mp - 1, rows, half), bf16),
        pltpu.SemaphoreType.DMA((len(ARRAYS) * len(KINDS),)),
        pltpu.SemaphoreType.DMA((len(ARRAYS) * len(KINDS),)),
        pltpu.SemaphoreType.DMA((len(ARRAYS) + 1,)),
        pltpu.SemaphoreType.DMA((16,)),
        pltpu.SemaphoreType.DMA((16,)),
    ]
    out = pl.pallas_call(
        functools.partial(layer_kernel, dp, mp, kept_own),
        out_shape=jax.ShapeDtypeStruct((rows, width), bf16),
        in_specs=[hbm, vmem, vmem, hbm, hbm, vmem, hbm, vmem, hbm, vmem, vmem, vmem],
        out_specs=vmem,
        scratch_shapes=scratch,
        compiler_params=pltpu.CompilerParams(
            collective_id=3, has_side_effects=True, vmem_limit_bytes=60 * 2**20
        ),
        cost_estimate=pl.CostEstimate(flops=10**10, bytes_accessed=10**8, transcendentals=0),
        name="layer",
    )(
        tokens.reshape(rows, width),
        sizes,
        ln1_gain.reshape(1, width),
        qkv_weight,
        proj_weight.T,
        ln2_gain.reshape(1, width),
        fc1_weight,
        fc1_bias.reshape(1, hidden),
        fc2_weight.T,
        pair_source,
        pair_target,
        kept_order,
    )
    return out[None, :kept_own]


def solution(mesh):
    line_by_two = mesh.shape["dp"] == 8 and mesh.shape["mp"] == 4
    return jax.shard_map(
        whole_layer if line_by_two else shards,
        mesh=mesh,
        in_specs=(
            P("dp", "mp", None),
            P("dp", None),
            P(),
            P(None, "dp", "mp"),
            P("mp", "dp"),
            P(),
            P("dp", "mp"),
            P("mp"),
            P("mp", "dp"),
            P("dp", None),
            P("dp", None),
            P("dp", None),
        ),
        out_specs=P("dp", "mp", None),
        check_vma=False,
    )
```

```python
import functools
import math

import jax
import jax.numpy as jnp
from jax import lax
from jax.experimental import pallas as pl
from jax.experimental.pallas import tpu as pltpu
from jax.sharding import PartitionSpec as P

HEADS = 16


def layer_norm(values, gain):
    center = values - jnp.mean(values, axis=-1, keepdims=True)
    spread = jnp.mean(center * center, axis=-1, keepdims=True)
    return center * lax.rsqrt(spread + 1e-06) * gain


def powers(count):
    bits = []
    bit = 1
    while bit < count:
        bits.append(bit)
        bit *= 2
    return bits


def toggled(index, mask):
    for bit in powers(mask + 1):
        if mask & bit:
            index = index + bit * (1 - 2 * lax.rem(lax.div(index, bit), 2))
    return index


def greet(peers):
    barrier = pltpu.get_barrier_semaphore()
    for axis, peer in peers:
        pl.semaphore_signal(
            barrier, inc=1, device_id={axis: peer}, device_id_type=pl.DeviceIdType.MESH
        )
    pl.semaphore_wait(barrier, len(peers))


class Copies:
    def __init__(self, send, recv):
        self.send, self.recv, self.made = send, recv, []

    def start(self, source, target, axis, peer):
        number = len(self.made)
        copy = pltpu.make_async_remote_copy(
            src_ref=source,
            dst_ref=target,
            send_sem=self.send.at[number],
            recv_sem=self.recv.at[number],
            device_id={axis: peer},
            device_id_type=pl.DeviceIdType.MESH,
        )
        copy.start()
        self.made.append(copy)
        return copy


def rows_of(out, owner, rows):
    span = pl.ds(pl.multiple_of(owner * rows, 16), rows)
    if len(out.shape) == 3:
        return out.at[:, span, :]
    return out.at[span, :]


class Waits:
    def __init__(self):
        self.seen = set()

    def ready(self, copy):
        if id(copy) not in self.seen:
            copy.wait_recv()
            self.seen.add(id(copy))


def dp_peers(dp):
    me = lax.axis_index("dp")
    return me, toggled(me, 1), lax.rem(me + 2, dp), lax.rem(me + dp - 2, dp)


def start_dp(own, out, copies, dp):
    me, pair, after, before = dp_peers(dp)
    here = rows_of(out, me, own.shape[-2])
    return [copies.start(own, here, "dp", peer) for peer in (pair, after, before)]


def relay_dp(own, out, copies, waits, state, dp, step):
    me, pair, after, before = dp_peers(dp)
    ring = dp // 2
    rows = own.shape[-2]
    other, forward, backward = state
    block = rows_of(out, lax.rem(me - 2 * step + 2 * dp, dp), rows)
    waits.ready(forward)
    if step < ring // 2:
        state[1] = copies.start(block, block, "dp", after)
    copies.start(block, block, "dp", pair)
    if step < ring - step:
        block = rows_of(out, toggled(lax.rem(me + 2 * (step - 1), dp), 1), rows)
        waits.ready(other)
        state[0] = copies.start(block, block, "dp", before)
        if step + 1 < ring - step - 1:
            block = rows_of(out, lax.rem(me + 2 * step, dp), rows)
            waits.ready(backward)
            state[2] = copies.start(block, block, "dp", before)


def gather_kernel(dp, mp, *refs):
    own, out = refs[:2], refs[2:4]
    send, recv, local = refs[4:]
    at = lax.axis_index("mp")
    me, pair, after, before = dp_peers(dp)
    greet(
        [("mp", toggled(at, bit)) for bit in powers(mp)]
        + [("dp", pair), ("dp", after), ("dp", before)]
    )
    copies, waits = Copies(send, recv), Waits()
    heads = start_dp(own[1], out[1], copies, dp)
    mine = rows_of(out[0], at, own[0].shape[0])
    bits = list(reversed(powers(mp)))
    here = {bit: copies.start(own[0], mine, "mp", toggled(at, bit)) for bit in bits}
    stays = []
    for number, owner in ((0, at), (1, me)):
        keep = pltpu.make_async_copy(
            own[number], rows_of(out[number], owner, own[number].shape[-2]), local.at[number]
        )
        keep.start()
        stays.append(keep)
    relay_dp(own[1], out[1], copies, waits, heads, dp, 1)
    held = [0]
    for bit in bits:
        for k in list(held):
            if k:
                waits.ready(here[k])
                block = rows_of(out[0], toggled(at, k), own[0].shape[0])
                here[k ^ bit] = copies.start(block, block, "mp", toggled(at, bit))
            held.append(k ^ bit)
    for step in range(2, dp // 4 + 1):
        relay_dp(own[1], out[1], copies, waits, heads, dp, step)
    for copy in copies.made:
        waits.ready(copy)
        copy.wait_send()
    for keep in stays:
        keep.wait()


def gather_all(normed, heads):
    dp, mp = lax.axis_size("dp"), lax.axis_size("mp")
    total = (mp - 1) + (dp - 1)
    shapes = [
        (mp * normed.shape[0], normed.shape[1]),
        (dp * heads.shape[0], heads.shape[1]),
    ]
    return pl.pallas_call(
        functools.partial(gather_kernel, dp, mp),
        out_shape=[jax.ShapeDtypeStruct(shape, jnp.bfloat16) for shape in shapes],
        in_specs=[pl.BlockSpec(memory_space=pltpu.VMEM)] * 2,
        out_specs=[pl.BlockSpec(memory_space=pl.ANY)] * 2,
        scratch_shapes=[
            pltpu.SemaphoreType.DMA((total,)),
            pltpu.SemaphoreType.DMA((total,)),
            pltpu.SemaphoreType.DMA((2,)),
        ],
        compiler_params=pltpu.CompilerParams(collective_id=0, has_side_effects=True),
        cost_estimate=pl.CostEstimate(
            flops=10**10, bytes_accessed=10**8, transcendentals=0
        ),
        name="gather_all",
    )(normed, heads)


def reduce_kernel(dp, mp, last, *refs):
    if last:
        parts, extra, out, held, landing, send, recv = refs
    else:
        parts, extra, own, out, whole, weight, held, landing, normed, send, recv, local = refs
    at = lax.axis_index("mp")
    peers = [("mp", toggled(at, bit)) for bit in powers(mp)]
    if not last:
        peers += [("dp", peer) for peer in dp_peers(dp)[1:]]
    greet(peers)
    copies, waits = Copies(send, recv), Waits()
    slots = 0
    stored = {k: None for k in range(mp)}
    if not last:
        state = start_dp(own, weight, copies, dp)
        rest = pltpu.make_async_copy(
            own, rows_of(weight, lax.axis_index("dp"), own.shape[0]), local.at[1]
        )
        rest.start()

    def source(k):
        return parts.at[toggled(at, k)] if stored[k] is None else held.at[k]

    for bit in powers(mp):
        moving = [k for k in reversed(range(mp)) if k in stored and k & bit]
        flights = []
        for k in moving:
            flights.append(
                (k, slots, copies.start(source(k), landing.at[slots], "mp", toggled(at, bit)))
            )
            slots += 1
        for k, slot, copy in flights:
            waits.ready(copy)
            kept = k ^ bit
            total = source(kept)[...].astype(jnp.float32) + landing[slot].astype(jnp.float32)
            if 2 * bit < mp:
                held[kept] = total.astype(jnp.bfloat16)
                stored[kept] = True
            del stored[k]
        if not last and bit == 1:
            relay_dp(own, weight, copies, waits, state, dp, 1)
    if last:
        out[...] = (extra[...] + total).astype(out.dtype)
    else:
        out[...] = total
        normed[...] = layer_norm(total, extra[...]).astype(jnp.bfloat16)
        keep = pltpu.make_async_copy(normed, whole.at[at], local.at[0])
        keep.start()
        bits = list(reversed(powers(mp)))
        here = {
            bit: copies.start(normed, whole.at[at], "mp", toggled(at, bit)) for bit in bits
        }
        for step in range(2, dp // 4 + 1):
            relay_dp(own, weight, copies, waits, state, dp, step)
        near = [0]
        for bit in bits:
            for k in list(near):
                if k:
                    waits.ready(here[k])
                    block = whole.at[toggled(at, k)]
                    here[k ^ bit] = copies.start(block, block, "mp", toggled(at, bit))
                near.append(k ^ bit)
        keep.wait()
        rest.wait()
    for copy in copies.made:
        waits.ready(copy)
        copy.wait_send()


def reduce_parts(parts, extra, own=None):
    mp, rows, width = parts.shape
    dp = lax.axis_size("dp")
    last = own is None
    operands = [parts, extra] if last else [parts, extra, own]
    vmem = pl.BlockSpec(memory_space=pltpu.VMEM)
    out_shape = [
        jax.ShapeDtypeStruct((rows, width), jnp.bfloat16 if last else jnp.float32)
    ]
    out_specs = [vmem]
    scratch = [
        pltpu.VMEM((mp, rows, width), jnp.bfloat16),
        pltpu.VMEM((mp - 1, rows, width), jnp.bfloat16),
    ]
    total = mp - 1
    if not last:
        out_shape.append(jax.ShapeDtypeStruct((mp, rows, width), jnp.bfloat16))
        out_shape.append(jax.ShapeDtypeStruct((dp * own.shape[0], own.shape[1]), jnp.bfloat16))
        out_specs += [pl.BlockSpec(memory_space=pl.ANY)] * 2
        scratch.append(pltpu.VMEM((rows, width), jnp.bfloat16))
        total = 2 * total + dp - 1
    scratch += [pltpu.SemaphoreType.DMA((total,)), pltpu.SemaphoreType.DMA((total,))]
    if not last:
        scratch.append(pltpu.SemaphoreType.DMA((2,)))
    return pl.pallas_call(
        functools.partial(reduce_kernel, dp, mp, last),
        out_shape=out_shape,
        in_specs=[vmem] * len(operands),
        out_specs=out_specs,
        scratch_shapes=scratch,
        compiler_params=pltpu.CompilerParams(
            collective_id=2 if last else 1, has_side_effects=True
        ),
        cost_estimate=pl.CostEstimate(
            flops=10**10, bytes_accessed=10**8, transcendentals=0
        ),
        name="reduce_last" if last else "reduce_norm_gather",
    )(*operands)


def shards(
    tokens,
    sizes,
    ln1_gain,
    qkv_weight,
    proj_weight,
    ln2_gain,
    fc1_weight,
    fc1_bias,
    fc2_weight,
    pair_source,
    pair_target,
    kept_order,
):
    images, own_tokens, width = tokens.shape
    length = sizes.shape[1]
    kept_total = kept_order.shape[1]
    count = lax.axis_size("mp")
    me = lax.axis_index("mp")
    kept_own = kept_total // count
    padded = -(-kept_own // 16) * 16
    head_size = width // HEADS
    local_width = qkv_weight.shape[2]
    local_heads = local_width // head_size

    base = tokens.astype(jnp.float32)
    normed = layer_norm(base, ln1_gain).astype(jnp.bfloat16)
    whole, heads_whole = gather_all(
        normed.reshape(own_tokens, width),
        jnp.concatenate(
            [qkv_weight[0], qkv_weight[1], qkv_weight[2], proj_weight.T], axis=1
        ),
    )
    whole = whole[None]
    whole, heads_whole, late = lax.optimization_barrier((whole, heads_whole, fc1_weight))
    fc1 = lax.all_gather(late, "dp", axis=0, tiled=True)

    positions = jnp.arange(length, dtype=jnp.int32)
    order = jnp.pad(
        kept_order.reshape(images, count, kept_own),
        ((0, 0), (0, 0), (0, padded - kept_own)),
        constant_values=-1,
    ).reshape(images, count * padded)
    hits = positions[None, None, :] == pair_source[:, :, None]
    destination = positions[None, :] + jnp.sum(
        jnp.where(hits, pair_target[:, :, None] - positions[None, None, :], 0), axis=1
    )
    joins = order[:, :, None] == destination[:, None, :]
    shares = jnp.where(joins, sizes[:, None, :], 0.0)
    merged_size = jnp.sum(shares, axis=2, keepdims=True)
    shares = (shares / jnp.where(merged_size > 0, merged_size, 1.0)).astype(jnp.bfloat16)
    own_shares = lax.dynamic_slice_in_dim(shares, me * own_tokens, own_tokens, 2)

    projected = jnp.einsum(
        "ind,df->inf", whole, heads_whole[:, : 3 * local_width], preferred_element_type=jnp.float32
    ).astype(jnp.bfloat16)
    shaped = [
        projected[:, :, c * local_width : (c + 1) * local_width].reshape(
            images, length, local_heads, head_size
        )
        for c in range(3)
    ]
    size_bias = jnp.log(sizes)[:, None, None, :]
    block = min(512, length)
    outputs = []
    for begin in range(0, length, block):
        scores = (
            jnp.einsum(
                "iqhe,ikhe->ihqk",
                shaped[0][:, begin : begin + block],
                shaped[1],
                preferred_element_type=jnp.float32,
            )
            / math.sqrt(head_size)
            + size_bias
        )
        weights = jax.nn.softmax(scores, axis=-1).astype(jnp.bfloat16)
        outputs.append(
            jnp.einsum("ihqk,ikhe->iqhe", weights, shaped[2], preferred_element_type=jnp.float32)
            .astype(jnp.bfloat16)
            .reshape(images, block, local_width)
        )
    attended = jnp.concatenate(outputs, axis=1)

    joined = jnp.einsum(
        "ijn,ind->ijd", shares, attended, preferred_element_type=jnp.float32
    ).astype(jnp.bfloat16)

    left, right = lax.optimization_barrier(
        (
            jnp.concatenate([joined, own_shares], axis=2),
            jnp.concatenate([heads_whole[:, 3 * local_width :].T, tokens[0]], axis=0),
        )
    )
    parts = jnp.einsum("ijd,de->ije", left, right, preferred_element_type=jnp.float32)
    parts = parts.astype(jnp.bfloat16).reshape(count, padded, width)
    merged, gathered, fc2 = reduce_parts(parts, ln2_gain.reshape(1, width), fc2_weight.T)
    hidden_sum = jnp.einsum(
        "md,df->mf", gathered.reshape(count * padded, width), fc1,
        preferred_element_type=jnp.float32,
    )
    hidden = jax.nn.gelu(hidden_sum + fc1_bias).astype(jnp.bfloat16)
    partial_out = jnp.einsum("mf,df->md", hidden, fc2, preferred_element_type=jnp.float32)
    partial_out = partial_out.astype(jnp.bfloat16).reshape(count, padded, width)
    out = reduce_parts(partial_out, merged)[0]
    return out[None, :kept_own]


LOG2E = math.log2(math.e)
KINDS = ("E1", "E2", "Y4", "N1", "N2", "M1", "M2", "M3", "M4", "Y1", "Y2", "Y3")
ARRAYS = ("kv0", "kv1", "pq0", "pq1", "f1a", "f1b", "f2a", "f2b")

SCHEDULE = {
    "ln": ((("s0", "kv0"), ("s0", "kv1"), ("s0", "pq0")), (("s0", "kv0"), ("s0", "kv1"), ("s0", "pq0"))),
    "tb": ((("s0", "pq1"), ("M1", "kv0"), ("M1", "pq0"), ("Y1", "pq0"), ("M1", "pq1"), ("M1", "kv1"), ("M2", "kv0"), ("Y1", "kv1"), ("M2", "kv1")), (("s0", "pq1"), ("N1", "kv0"), ("E1", "kv0"), ("E1", "kv1"), ("N1", "kv1"), ("N1", "pq0"), ("E1", "pq1"), ("N1", "pq1"), ("E1", "pq0"), ("N2", "kv0"), ("Y1", "kv1"), ("Y1", "pq1"), ("N2", "kv1"))),
    "tk": ((("M2", "pq0"),), (("N2", "pq1"),)),
    "w0": ((("M2", "pq1"), ("Y1", "kv0"), ("M3", "kv0"), ("Y1", "pq1"), ("s0", "f1a"), ("M3", "kv1"), ("M3", "pq1"), ("M3", "pq0")), (("N2", "pq0"), ("Y1", "pq0"), ("Y1", "kv0"), ("s0", "f1a"))),
    "w1": ((("s0", "f1b"),), ()),
    "sr": ((("M1", "f1a"),), (("N1", "f1a"),)),
    "a0": ((("M2", "f1a"),), (("E1", "f1a"),)),
    "a1": ((), (("s0", "f1b"),)),
    "a3": ((("Y1", "f1b"),), ()),
    "a4": ((("s0", "f2a"),), ()),
    "a6": ((("Y1", "f1a"),), ()),
    "a7": ((), (("N2", "f1a"),)),
    "r1": ((("M3", "f1a"),), ()),
    "a10": ((("M1", "f1b"),), (("N1", "f1b"),)),
    "a11": ((("M2", "f1b"),), (("E1", "f1b"),)),
    "a12": ((("Y1", "f2a"),), (("s0", "f2a"),)),
    "a14": ((), (("Y1", "f1b"),)),
    "a15": ((), (("Y1", "f1a"),)),
    "rr": ((("s0", "f2b"), ("M3", "f1b")), (("N2", "f1b"), ("N1", "f2a"), ("E1", "f2a"))),
    "nm": ((("Y1", "f2b"), ("M2", "f2a")), ()),
    "e0": ((("M1", "f2b"),), ()),
    "e1": ((("M1", "f2a"), ("M3", "f2a")), (("s0", "f2b"), ("N2", "f2a"), ("Y1", "f2b"), ("N1", "f2b"), ("Y1", "f2a"), ("E1", "f2b"))),
    "e2": ((("M2", "f2b"),), ()),
    "na": ((("M3", "f2b"),), (("N2", "f2b"),)),
}


def nt_dot(left, right):
    return lax.dot_general(
        left, right, (((1,), (1,)), ((), ())), preferred_element_type=jnp.float32
    )


START = ((("E1", "inner"), ("Y1", "pair")), (("M1", "outer"), ("N1", "inner"), ("Y1", "pair")))
RELAY = {
    (0, "M1"): (("Y4", 1, "pair", 0),),
    (0, "Y1"): (("E2", "pair", "inner", None),),
    (0, "M2"): (("Y2", 2, "pair", None),),
    (0, "M3"): (("Y3", 3, "pair", None),),
    (1, "N1"): (("M2", 1, "outer", None), ("Y2", 1, "pair", None)),
    (1, "E1"): (("N2", "outer", "inner", None),),
    (1, "Y1"): (("M4", "pair", "outer", 1),),
    (1, "N2"): (("M3", 2, "outer", None), ("Y3", 2, "pair", None)),
}


class Streams:
    def __init__(self, dp, homes, send, recv, local):
        me = lax.axis_index("dp")
        z, y = lax.div(me, 2), lax.rem(me, 2)
        high = lax.div(z, 2)
        step = 1 - 2 * high
        self.end = lax.rem(lax.div(z + 1, 2), 2) == 0
        self.mid = lax.rem(lax.div(z + 1, 2), 2) == 1
        self.me = me
        self.pair = z * 2 + 1 - y
        self.inner = (z + step) * 2 + y
        self.outer = lax.rem((z - step) * 2 + y + dp, dp)
        middle = lax.rem(lax.div(z + 1, 2), 2)
        self.far = [(z + step * (k - middle)) * 2 for k in (2, 3)]
        self.ahead = [lax.rem((z + step * k) * 2 + y + dp, dp) for k in range(4)]
        self.homes, self.send, self.recv, self.local = homes, send, recv, local
        self.peers = {"inner": self.inner, "outer": self.outer, "pair": self.pair}

    def block(self, name, owner, part=None):
        _, target, stride, low, count = self.homes[name]
        if part is not None:
            first = -(-count // 32) * 16
            low, count = low + part * first, (first, count - first)[part]
        return target(pl.ds(pl.multiple_of(owner * stride + low, 16), count))

    def own(self, name):
        return self.homes[name][0]

    def copy(self, name, kind, source, target, peer):
        number = ARRAYS.index(name) * len(KINDS) + KINDS.index(kind)
        return pltpu.make_async_remote_copy(
            src_ref=source,
            dst_ref=target,
            send_sem=self.send.at[number],
            recv_sem=self.recv.at[number],
            device_id={"dp": self.peers[peer]},
            device_id_type=pl.DeviceIdType.MESH,
        )

    def move(self, name, kind, owner, peer, part=None):
        block = self.block(name, owner, part)
        self.copy(name, kind, block, block, peer).start()

    def arrived(self, name, *kinds):
        for kind in kinds:
            block = self.block(name, self.me, {"Y4": 0, "M4": 1}.get(kind))
            self.copy(name, kind, block, block, "pair").wait_recv()

    def stay(self, name):
        return pltpu.make_async_copy(
            self.own(name), self.block(name, self.me), self.local.at[ARRAYS.index(name)]
        )

    def act(self, role, what, name):
        if what == "s0":
            here = self.block(name, self.me)
            for kind, peer in START[role]:
                own = here if self.own(name) is None else self.own(name)
                self.copy(name, kind, own, here, peer).start()
            if self.own(name) is not None:
                self.stay(name).start()
            return
        self.arrived(name, what)
        for kind, owner, peer, part in RELAY[role, what]:
            who = {"pair": self.pair, "outer": self.outer}.get(owner)
            self.move(name, kind, self.ahead[owner] if who is None else who, peer, part)

    def serve(self, point, when=None):
        for role, here in ((0, self.end), (1, self.mid)):
            todo = SCHEDULE.get(point, ((), ()))[role]
            if todo:
                condition = here if when is None else jnp.logical_and(when, here)

                @pl.when(condition)
                def _():
                    for what, name in todo:
                        self.act(role, what, name)

    def near(self, name):
        if self.own(name) is not None:
            self.stay(name).wait()

        @pl.when(self.end)
        def _():
            self.arrived(name, "M4", "Y4")

        @pl.when(self.mid)
        def _():
            self.arrived(name, "E2")

    def full(self, name):
        self.near(name)
        self.arrived(name, "Y2", "Y3")

    def sent(self, name):
        def drain(*kinds):
            for kind in kinds:
                block = self.block(name, self.me, {"Y4": 0, "M4": 1}.get(kind))
                self.copy(name, kind, block, block, "pair").wait_send()

        drain("Y1", "Y2", "Y3")

        @pl.when(self.end)
        def _():
            drain("E1", "E2", "Y4")

        @pl.when(self.mid)
        def _():
            drain("N1", "N2", "M1", "M2", "M3", "M4")


def column_of(row, count):
    down = lax.broadcasted_iota(jnp.int32, (count, count), 0)
    over = lax.broadcasted_iota(jnp.int32, (count, count), 1)
    return jnp.sum(jnp.where(down == over, row, 0.0), axis=1, keepdims=True)


def layer_kernel(dp, mp, kept_own, *refs):
    (tokens, sizes, gain_one, qkv, proj, gain_two, fc1, bias, fc2, source, target, order) = refs[:12]
    out = refs[12]
    (tok, raw_qkv, raw_proj, whole, wkv, wpq, w1, w2, shares, picks, own_share, source_share,
     kbuf, vbuf, qall, qbuf, source_att, attb, joined, parts, landing, merged, again, hidden,
     near_parts, near_landing, far_parts, far_landing, far_own,
     send, recv, local, msend, mrecv) = refs[13:]
    rows, width = tok.shape
    length = sizes.shape[1]
    local_width = joined.shape[1]
    local_heads, _, lanes = kbuf.shape
    head_size = local_width // local_heads
    half = width // 2
    at = lax.axis_index("mp")
    block_of = [toggled(at, k) for k in range(mp)]
    pair, across = block_of[1], block_of[2]

    cut = fc1.shape[1] // 2
    shard = fc1.shape[0]
    homes = {
        "kv0": (None, lambda r: wkv.at[r, :], shard, 0, shard // 2),
        "kv1": (None, lambda r: wkv.at[r, :], shard, shard // 2, shard // 2),
        "pq0": (None, lambda r: wpq.at[r, :], shard, 0, shard // 2),
        "pq1": (None, lambda r: wpq.at[r, :], shard, shard // 2, shard // 2),
        "f1a": (fc1.at[:, pl.ds(0, cut)], lambda r: w1.at[r, pl.ds(0, cut)], shard, 0, shard),
        "f1b": (fc1.at[:, pl.ds(cut, cut)], lambda r: w1.at[r, pl.ds(cut, cut)], shard, 0, shard),
        "f2a": (fc2.at[:, pl.ds(0, cut)], lambda r: w2.at[r, pl.ds(0, cut)], shard, 0, shard),
        "f2b": (fc2.at[:, pl.ds(cut, cut)], lambda r: w2.at[r, pl.ds(cut, cut)], shard, 0, shard),
    }
    st = Streams(dp, homes, send, recv, local)

    load = pltpu.make_async_copy(tokens, tok, local.at[len(ARRAYS)])
    load.start()
    load_qkv = pltpu.make_async_copy(qkv, raw_qkv, local.at[len(ARRAYS) + 1])
    load_qkv.start()
    load_proj = pltpu.make_async_copy(proj, raw_proj, local.at[len(ARRAYS) + 2])
    load_proj.start()

    barrier = pltpu.get_barrier_semaphore()

    def hello(axis, peer):
        pl.semaphore_signal(
            barrier, inc=1, device_id={axis: peer}, device_id_type=pl.DeviceIdType.MESH
        )

    hello("dp", st.pair)
    hello("dp", st.inner)
    hello("mp", pair)
    hello("mp", across)

    @pl.when(st.mid)
    def _():
        hello("dp", st.outer)

    load_qkv.wait()
    load_proj.wait()
    mine = pl.ds(pl.multiple_of(st.me * shard, shard), shard)
    wkv[mine, 0:local_width] = raw_qkv[1]
    wkv[mine, local_width : 2 * local_width] = raw_qkv[2]
    wpq[mine, 0:local_width] = raw_proj[...]
    wpq[mine, local_width : 2 * local_width] = raw_qkv[0]

    @pl.when(st.end)
    def _():
        pl.semaphore_wait(barrier, 4)

    @pl.when(st.mid)
    def _():
        pl.semaphore_wait(barrier, 5)

    st.serve("go")

    made = []

    def give(src, dst, peer):
        copy = pltpu.make_async_remote_copy(
            src_ref=src,
            dst_ref=dst,
            send_sem=msend.at[len(made)],
            recv_sem=mrecv.at[len(made)],
            device_id={"mp": peer},
            device_id_type=pl.DeviceIdType.MESH,
        )
        copy.start()
        made.append(copy)
        return copy

    load.wait()
    slab = 32
    first_gain = gain_one[...].reshape(1, width)
    second_gain = gain_two[...].reshape(1, width)
    first_bias = bias[...].reshape(1, bias.shape[0])

    def norm_rows(i, carry):
        span = pl.ds(pl.multiple_of(i * slab, slab), slab)
        whole[at, span, :] = layer_norm(
            tok[span, :].astype(jnp.float32), first_gain
        ).astype(jnp.bfloat16)
        return carry

    lax.fori_loop(0, rows // slab, norm_rows, 0)
    token_pair = give(whole.at[at], whole.at[at], pair)
    token_across = give(whole.at[at], whole.at[at], across)
    st.serve("ln")

    position = lax.broadcasted_iota(jnp.int32, (1, length), 1).astype(jnp.float32)
    count = source.shape[1]
    source_column = column_of(source[...].astype(jnp.float32), count)
    target_column = column_of(target[...].astype(jnp.float32), count)
    destination = position + jnp.sum(
        jnp.where(position == source_column, target_column - position, 0.0),
        axis=0,
        keepdims=True,
    )
    size_row = sizes[...]
    order_row = order[...].astype(jnp.float32)

    picked = (position == source_column).astype(jnp.bfloat16)

    def table(b, carry):
        shape = (rows, order.shape[1])
        down = lax.broadcasted_iota(jnp.int32, shape, 0)
        over = lax.broadcasted_iota(jnp.int32, shape, 1)
        mine = jnp.logical_and(over == down + b * kept_own, down < kept_own)
        wanted = jnp.sum(jnp.where(mine, order_row + 1.0, 0.0), axis=1, keepdims=True) - 1.0
        share = jnp.where(wanted == destination, size_row, 0.0)
        total = jnp.sum(share, axis=1, keepdims=True)
        share = share / jnp.where(total > 0, total, 1.0)
        shares[b] = share.astype(jnp.bfloat16)
        here = wanted == position
        picks[b] = jnp.where(here, 1.0, 0.0).astype(jnp.bfloat16)
        own_share[b] = jnp.sum(jnp.where(here, share, 0.0), axis=1, keepdims=True)
        source_share[b] = nt_dot(share.astype(jnp.bfloat16), picked).astype(jnp.bfloat16)
        return carry

    lax.fori_loop(0, mp, table, 0)
    lane = lax.broadcasted_iota(jnp.int32, (length, lanes), 1)
    for h in range(local_heads):
        kbuf[h] = jnp.zeros((length, lanes), jnp.bfloat16)
        qbuf[h] = jnp.zeros((rows, lanes), jnp.bfloat16)
        vbuf[h] = jnp.where(lane == head_size, 1.0, 0.0).astype(jnp.bfloat16)
    size_bias = jnp.log(size_row) * LOG2E

    st.serve("tb")
    token_across.wait_recv()
    token_far = give(whole.at[across], whole.at[across], pair)
    st.serve("tk")
    token_pair.wait_recv()
    token_far.wait_recv()

    def project_kv(b, carry):
        product = jnp.dot(whole[b], wkv[...], preferred_element_type=jnp.float32)
        product = product.astype(jnp.bfloat16)
        span = pl.ds(pl.multiple_of(b * rows, rows), rows)
        for h in range(local_heads):
            low = h * head_size
            kbuf[h, span, 0:head_size] = product[:, low : low + head_size]
            low = low + local_width
            vbuf[h, span, 0:head_size] = product[:, low : low + head_size]
        return carry

    skip = local_width % 128
    factor = LOG2E / math.sqrt(head_size)

    def project_q(b, carry):
        product = jnp.dot(
            whole[b], wpq[:, local_width - skip :], preferred_element_type=jnp.float32
        )
        span = pl.ds(pl.multiple_of(b * rows, rows), rows)
        qall[span, :] = (product * factor).astype(jnp.bfloat16)
        return carry

    st.serve("w0")
    st.full("kv0")
    st.full("kv1")
    lax.fori_loop(0, mp, project_kv, 0)
    st.serve("w1")
    st.full("pq0")
    st.full("pq1")
    lax.fori_loop(0, mp, project_q, 0)

    def heads_of(product):
        chosen = product.astype(jnp.bfloat16)
        for h in range(local_heads):
            low = skip + h * head_size
            yield h, chosen[:, low : low + head_size]

    def mix(query, h):
        scores = nt_dot(query, kbuf[h]) + size_bias
        top = jnp.max(scores, axis=1, keepdims=True)
        weights = jnp.exp2(scores - top).astype(jnp.bfloat16)
        mixed = jnp.dot(weights, vbuf[h], preferred_element_type=jnp.float32)
        return mixed / mixed[:, head_size : head_size + 1]

    st.serve("sr")
    product = jnp.dot(picked, qall[...], preferred_element_type=jnp.float32)
    for h, query in heads_of(product):
        qbuf[h, 0:count, 0:head_size] = query

    def attend_source(h, carry):
        source_att[h] = mix(qbuf[h, 0:count, :], h).astype(jnp.bfloat16)
        return carry

    lax.fori_loop(0, local_heads, attend_source, 0)

    def part_of(turn, block):
        product = jnp.dot(picks[block], qall[...], preferred_element_type=jnp.float32)
        for h, query in heads_of(product):
            qbuf[h, :, 0:head_size] = query

        def attend(h, carry):
            for n in range(local_heads):
                st.serve(f"a{turn * local_heads + n}", h == n)
            taken = jnp.dot(
                source_share[block], source_att[h], preferred_element_type=jnp.float32
            )
            attb[h] = (mix(qbuf[h], h) * own_share[block] + taken).astype(jnp.bfloat16)
            return carry

        lax.fori_loop(0, local_heads, attend, 0)
        for h in range(local_heads):
            joined[:, h * head_size : (h + 1) * head_size] = attb[h, :, 0:head_size]
        st.serve(f"r{turn}")
        kept = shares[block, :, pl.ds(pl.multiple_of(at * rows, rows), rows)]
        return nt_dot(joined[...], wpq[:, 0:local_width]) + jnp.dot(
            kept, tok[...], preferred_element_type=jnp.float32
        )

    parts[2] = part_of(0, block_of[3]).astype(jnp.bfloat16)
    first = give(parts.at[2], landing.at[2], pair)
    total = part_of(1, across)
    first.wait_recv()
    parts[1] = (total + landing[2].astype(jnp.float32)).astype(jnp.bfloat16)
    second = give(parts.at[1], landing.at[1], across)
    parts[0] = part_of(2, pair).astype(jnp.bfloat16)
    third = give(parts.at[0], landing.at[0], pair)
    merged[...] = part_of(3, at)
    st.serve("rr")
    third.wait_recv()
    second.wait_recv()

    def norm_again(i, carry):
        span = pl.ds(pl.multiple_of(i * slab, slab), slab)
        total = (
            merged[span, :]
            + landing[0, span, :].astype(jnp.float32)
            + landing[1, span, :].astype(jnp.float32)
        )
        merged[span, :] = total
        again[at, span, :] = layer_norm(total, second_gain).astype(jnp.bfloat16)
        return carry

    lax.fori_loop(0, rows // slab, norm_again, 0)
    norm_pair = give(again.at[at], again.at[at], pair)
    norm_across = give(again.at[at], again.at[at], across)
    st.serve("nm")
    st.full("f1a")
    st.full("f1b")

    def expand(block):
        product = jnp.dot(again[block], w1[...], preferred_element_type=jnp.float32)
        hidden[block] = jax.nn.gelu(product + first_bias).astype(jnp.bfloat16)

    expand(at)
    st.serve("e0")
    norm_pair.wait_recv()
    expand(pair)
    st.serve("e1")
    norm_across.wait_recv()
    norm_far = give(again.at[across], again.at[across], pair)
    st.serve("ag")
    expand(across)
    st.serve("e2")
    norm_far.wait_recv()
    expand(block_of[3])
    st.serve("e3")

    near = lax.div(lax.div(st.me, 2), 2)

    def shrink(start, size, ready, landed):
        columns = pl.ds(pl.multiple_of(start, shard), size)

        def piece(block):
            return nt_dot(hidden[block], w2[columns, :])

        ready[2] = piece(block_of[3]).astype(jnp.bfloat16)
        one = give(ready.at[2], landed.at[2], pair)
        total = piece(across)
        one.wait_recv()
        ready[1] = (total + landed[2].astype(jnp.float32)).astype(jnp.bfloat16)
        two = give(ready.at[1], landed.at[1], across)
        ready[0] = piece(pair).astype(jnp.bfloat16)
        three = give(ready.at[0], landed.at[0], pair)
        return piece(at), two, three

    def landed_sum(landed):
        return landed[0].astype(jnp.float32) + landed[1].astype(jnp.float32)

    st.near("f2a")
    st.near("f2b")
    span = pl.ds(pl.multiple_of(near * half, half), half)
    total, *close = shrink(near * half, half, near_parts, near_landing)
    merged[:, span] = merged[:, span] + total
    st.serve("na")
    flights = []
    for number, kind in ((0, "Y2"), (1, "Y3")):
        st.arrived("f2a", kind)
        st.arrived("f2b", kind)
        total, *flight = shrink(
            lax.div(st.far[number], 2) * 2 * shard, 2 * shard, far_parts.at[number],
            far_landing.at[number],
        )
        far_own[number] = total
        flights += flight
        st.serve(("nc", "nd")[number])
    for flight in close:
        flight.wait_recv()
    out[:, span] = (merged[:, span] + landed_sum(near_landing)).astype(out.dtype)
    for flight in flights:
        flight.wait_recv()
    span = pl.ds(pl.multiple_of((1 - near) * half, half), half)
    sides = [
        far_own[side] + landed_sum(far_landing.at[side]) for side in (near, 1 - near)
    ]
    out[:, span] = (merged[:, span] + jnp.concatenate(sides, axis=1)).astype(out.dtype)
    for name in ARRAYS:
        st.sent(name)
    for copy in made:
        copy.wait_send()


def whole_layer(tokens, sizes, ln1_gain, qkv_weight, proj_weight, ln2_gain, fc1_weight, fc1_bias,
                fc2_weight, pair_source, pair_target, kept_order):
    dp, mp = lax.axis_size("dp"), lax.axis_size("mp")
    _, rows, width = tokens.shape
    length = sizes.shape[1]
    kept_own = kept_order.shape[1] // mp
    local_width = qkv_weight.shape[2]
    local_heads = HEADS * local_width // width
    head_size = local_width // local_heads
    lanes = -(-(head_size + 1) // 128) * 128
    hidden = fc1_weight.shape[1]
    bf16, f32 = jnp.bfloat16, jnp.float32
    vmem = pl.BlockSpec(memory_space=pltpu.VMEM)
    hbm = pl.BlockSpec(memory_space=pl.ANY)
    half = width // 2
    shard, count = fc1_weight.shape[0], pair_source.shape[1]
    whole_q = local_width + local_width % 128
    scratch = [
        pltpu.VMEM((rows, width), bf16),
        pltpu.VMEM((3, shard, local_width), bf16),
        pltpu.VMEM((shard, local_width), bf16),
        pltpu.VMEM((mp, rows, width), bf16),
        pltpu.VMEM((width, 2 * local_width), bf16),
        pltpu.VMEM((width, 2 * local_width), bf16),
        pltpu.VMEM((width, hidden), bf16),
        pltpu.VMEM((width, hidden), bf16),
        pltpu.VMEM((mp, rows, length), bf16),
        pltpu.VMEM((mp, rows, length), bf16),
        pltpu.VMEM((mp, rows, 1), f32),
        pltpu.VMEM((mp, rows, count), bf16),
        pltpu.VMEM((local_heads, length, lanes), bf16),
        pltpu.VMEM((local_heads, length, lanes), bf16),
        pltpu.VMEM((length, whole_q), bf16),
        pltpu.VMEM((local_heads, rows, lanes), bf16),
        pltpu.VMEM((local_heads, count, lanes), bf16),
        pltpu.VMEM((local_heads, rows, lanes), bf16),
        pltpu.VMEM((rows, local_width), bf16),
        pltpu.VMEM((mp - 1, rows, width), bf16),
        pltpu.VMEM((mp - 1, rows, width), bf16),
        pltpu.VMEM((rows, width), f32),
        pltpu.VMEM((mp, rows, width), bf16),
        pltpu.VMEM((mp, rows, hidden), bf16),
        pltpu.VMEM((mp - 1, rows, half), bf16),
        pltpu.VMEM((mp - 1, rows, half), bf16),
        pltpu.VMEM((2, mp - 1, rows, 2 * shard), bf16),
        pltpu.VMEM((2, mp - 1, rows, 2 * shard), bf16),
        pltpu.VMEM((2, rows, 2 * shard), f32),
        pltpu.SemaphoreType.DMA((len(ARRAYS) * len(KINDS),)),
        pltpu.SemaphoreType.DMA((len(ARRAYS) * len(KINDS),)),
        pltpu.SemaphoreType.DMA((len(ARRAYS) + 3,)),
        pltpu.SemaphoreType.DMA((18,)),
        pltpu.SemaphoreType.DMA((18,)),
    ]
    out = pl.pallas_call(
        functools.partial(layer_kernel, dp, mp, kept_own),
        out_shape=jax.ShapeDtypeStruct((rows, width), bf16),
        in_specs=[hbm, vmem, vmem, hbm, hbm, vmem, hbm, vmem, hbm, vmem, vmem, vmem],
        out_specs=vmem,
        scratch_shapes=scratch,
        compiler_params=pltpu.CompilerParams(
            collective_id=3, has_side_effects=True, vmem_limit_bytes=60 * 2**20
        ),
        cost_estimate=pl.CostEstimate(flops=10**10, bytes_accessed=10**8, transcendentals=0),
        name="layer",
    )(
        tokens.reshape(rows, width),
        sizes,
        ln1_gain,
        qkv_weight,
        proj_weight.T,
        ln2_gain,
        fc1_weight,
        fc1_bias,
        fc2_weight.T,
        pair_source,
        pair_target,
        kept_order,
    )
    return out[None, :kept_own]


def solution(mesh):
    line_by_two = mesh.shape["dp"] == 8 and mesh.shape["mp"] == 4
    return jax.shard_map(
        whole_layer if line_by_two else shards,
        mesh=mesh,
        in_specs=(
            P("dp", "mp", None),
            P("dp", None),
            P(),
            P(None, "dp", "mp"),
            P("mp", "dp"),
            P(),
            P("dp", "mp"),
            P("mp"),
            P("mp", "dp"),
            P("dp", None),
            P("dp", None),
            P("dp", None),
        ),
        out_specs=P("dp", "mp", None),
        check_vma=False,
    )
```

```python
import functools
import math

import jax
import jax.numpy as jnp
from jax import lax
from jax.experimental import pallas as pl
from jax.experimental.pallas import tpu as pltpu
from jax.sharding import PartitionSpec as P

HEADS = 16


def layer_norm(values, gain):
    center = values - jnp.mean(values, axis=-1, keepdims=True)
    spread = jnp.mean(center * center, axis=-1, keepdims=True)
    return center * lax.rsqrt(spread + 1e-06) * gain


def powers(count):
    bits = []
    bit = 1
    while bit < count:
        bits.append(bit)
        bit *= 2
    return bits


def toggled(index, mask):
    for bit in powers(mask + 1):
        if mask & bit:
            index = index + bit * (1 - 2 * lax.rem(lax.div(index, bit), 2))
    return index


def greet(peers):
    barrier = pltpu.get_barrier_semaphore()
    for axis, peer in peers:
        pl.semaphore_signal(
            barrier, inc=1, device_id={axis: peer}, device_id_type=pl.DeviceIdType.MESH
        )
    pl.semaphore_wait(barrier, len(peers))


class Copies:
    def __init__(self, send, recv):
        self.send, self.recv, self.made = send, recv, []

    def start(self, source, target, axis, peer):
        number = len(self.made)
        copy = pltpu.make_async_remote_copy(
            src_ref=source,
            dst_ref=target,
            send_sem=self.send.at[number],
            recv_sem=self.recv.at[number],
            device_id={axis: peer},
            device_id_type=pl.DeviceIdType.MESH,
        )
        copy.start()
        self.made.append(copy)
        return copy


def rows_of(out, owner, rows):
    span = pl.ds(pl.multiple_of(owner * rows, 16), rows)
    if len(out.shape) == 3:
        return out.at[:, span, :]
    return out.at[span, :]


class Waits:
    def __init__(self):
        self.seen = set()

    def ready(self, copy):
        if id(copy) not in self.seen:
            copy.wait_recv()
            self.seen.add(id(copy))


def dp_peers(dp):
    me = lax.axis_index("dp")
    return me, toggled(me, 1), lax.rem(me + 2, dp), lax.rem(me + dp - 2, dp)


def start_dp(own, out, copies, dp):
    me, pair, after, before = dp_peers(dp)
    here = rows_of(out, me, own.shape[-2])
    return [copies.start(own, here, "dp", peer) for peer in (pair, after, before)]


def relay_dp(own, out, copies, waits, state, dp, step):
    me, pair, after, before = dp_peers(dp)
    ring = dp // 2
    rows = own.shape[-2]
    other, forward, backward = state
    block = rows_of(out, lax.rem(me - 2 * step + 2 * dp, dp), rows)
    waits.ready(forward)
    if step < ring // 2:
        state[1] = copies.start(block, block, "dp", after)
    copies.start(block, block, "dp", pair)
    if step < ring - step:
        block = rows_of(out, toggled(lax.rem(me + 2 * (step - 1), dp), 1), rows)
        waits.ready(other)
        state[0] = copies.start(block, block, "dp", before)
        if step + 1 < ring - step - 1:
            block = rows_of(out, lax.rem(me + 2 * step, dp), rows)
            waits.ready(backward)
            state[2] = copies.start(block, block, "dp", before)


def gather_kernel(dp, mp, *refs):
    own, out = refs[:2], refs[2:4]
    send, recv, local = refs[4:]
    at = lax.axis_index("mp")
    me, pair, after, before = dp_peers(dp)
    greet(
        [("mp", toggled(at, bit)) for bit in powers(mp)]
        + [("dp", pair), ("dp", after), ("dp", before)]
    )
    copies, waits = Copies(send, recv), Waits()
    heads = start_dp(own[1], out[1], copies, dp)
    mine = rows_of(out[0], at, own[0].shape[0])
    bits = list(reversed(powers(mp)))
    here = {bit: copies.start(own[0], mine, "mp", toggled(at, bit)) for bit in bits}
    stays = []
    for number, owner in ((0, at), (1, me)):
        keep = pltpu.make_async_copy(
            own[number], rows_of(out[number], owner, own[number].shape[-2]), local.at[number]
        )
        keep.start()
        stays.append(keep)
    relay_dp(own[1], out[1], copies, waits, heads, dp, 1)
    held = [0]
    for bit in bits:
        for k in list(held):
            if k:
                waits.ready(here[k])
                block = rows_of(out[0], toggled(at, k), own[0].shape[0])
                here[k ^ bit] = copies.start(block, block, "mp", toggled(at, bit))
            held.append(k ^ bit)
    for step in range(2, dp // 4 + 1):
        relay_dp(own[1], out[1], copies, waits, heads, dp, step)
    for copy in copies.made:
        waits.ready(copy)
        copy.wait_send()
    for keep in stays:
        keep.wait()


def gather_all(normed, heads):
    dp, mp = lax.axis_size("dp"), lax.axis_size("mp")
    total = (mp - 1) + (dp - 1)
    shapes = [
        (mp * normed.shape[0], normed.shape[1]),
        (dp * heads.shape[0], heads.shape[1]),
    ]
    return pl.pallas_call(
        functools.partial(gather_kernel, dp, mp),
        out_shape=[jax.ShapeDtypeStruct(shape, jnp.bfloat16) for shape in shapes],
        in_specs=[pl.BlockSpec(memory_space=pltpu.VMEM)] * 2,
        out_specs=[pl.BlockSpec(memory_space=pl.ANY)] * 2,
        scratch_shapes=[
            pltpu.SemaphoreType.DMA((total,)),
            pltpu.SemaphoreType.DMA((total,)),
            pltpu.SemaphoreType.DMA((2,)),
        ],
        compiler_params=pltpu.CompilerParams(collective_id=0, has_side_effects=True),
        cost_estimate=pl.CostEstimate(
            flops=10**10, bytes_accessed=10**8, transcendentals=0
        ),
        name="gather_all",
    )(normed, heads)


def reduce_kernel(dp, mp, last, *refs):
    if last:
        parts, extra, out, held, landing, send, recv = refs
    else:
        parts, extra, own, out, whole, weight, held, landing, normed, send, recv, local = refs
    at = lax.axis_index("mp")
    peers = [("mp", toggled(at, bit)) for bit in powers(mp)]
    if not last:
        peers += [("dp", peer) for peer in dp_peers(dp)[1:]]
    greet(peers)
    copies, waits = Copies(send, recv), Waits()
    slots = 0
    stored = {k: None for k in range(mp)}
    if not last:
        state = start_dp(own, weight, copies, dp)
        rest = pltpu.make_async_copy(
            own, rows_of(weight, lax.axis_index("dp"), own.shape[0]), local.at[1]
        )
        rest.start()

    def source(k):
        return parts.at[toggled(at, k)] if stored[k] is None else held.at[k]

    for bit in powers(mp):
        moving = [k for k in reversed(range(mp)) if k in stored and k & bit]
        flights = []
        for k in moving:
            flights.append(
                (k, slots, copies.start(source(k), landing.at[slots], "mp", toggled(at, bit)))
            )
            slots += 1
        for k, slot, copy in flights:
            waits.ready(copy)
            kept = k ^ bit
            total = source(kept)[...].astype(jnp.float32) + landing[slot].astype(jnp.float32)
            if 2 * bit < mp:
                held[kept] = total.astype(jnp.bfloat16)
                stored[kept] = True
            del stored[k]
        if not last and bit == 1:
            relay_dp(own, weight, copies, waits, state, dp, 1)
    if last:
        out[...] = (extra[...] + total).astype(out.dtype)
    else:
        out[...] = total
        normed[...] = layer_norm(total, extra[...]).astype(jnp.bfloat16)
        keep = pltpu.make_async_copy(normed, whole.at[at], local.at[0])
        keep.start()
        bits = list(reversed(powers(mp)))
        here = {
            bit: copies.start(normed, whole.at[at], "mp", toggled(at, bit)) for bit in bits
        }
        for step in range(2, dp // 4 + 1):
            relay_dp(own, weight, copies, waits, state, dp, step)
        near = [0]
        for bit in bits:
            for k in list(near):
                if k:
                    waits.ready(here[k])
                    block = whole.at[toggled(at, k)]
                    here[k ^ bit] = copies.start(block, block, "mp", toggled(at, bit))
                near.append(k ^ bit)
        keep.wait()
        rest.wait()
    for copy in copies.made:
        waits.ready(copy)
        copy.wait_send()


def reduce_parts(parts, extra, own=None):
    mp, rows, width = parts.shape
    dp = lax.axis_size("dp")
    last = own is None
    operands = [parts, extra] if last else [parts, extra, own]
    vmem = pl.BlockSpec(memory_space=pltpu.VMEM)
    out_shape = [
        jax.ShapeDtypeStruct((rows, width), jnp.bfloat16 if last else jnp.float32)
    ]
    out_specs = [vmem]
    scratch = [
        pltpu.VMEM((mp, rows, width), jnp.bfloat16),
        pltpu.VMEM((mp - 1, rows, width), jnp.bfloat16),
    ]
    total = mp - 1
    if not last:
        out_shape.append(jax.ShapeDtypeStruct((mp, rows, width), jnp.bfloat16))
        out_shape.append(jax.ShapeDtypeStruct((dp * own.shape[0], own.shape[1]), jnp.bfloat16))
        out_specs += [pl.BlockSpec(memory_space=pl.ANY)] * 2
        scratch.append(pltpu.VMEM((rows, width), jnp.bfloat16))
        total = 2 * total + dp - 1
    scratch += [pltpu.SemaphoreType.DMA((total,)), pltpu.SemaphoreType.DMA((total,))]
    if not last:
        scratch.append(pltpu.SemaphoreType.DMA((2,)))
    return pl.pallas_call(
        functools.partial(reduce_kernel, dp, mp, last),
        out_shape=out_shape,
        in_specs=[vmem] * len(operands),
        out_specs=out_specs,
        scratch_shapes=scratch,
        compiler_params=pltpu.CompilerParams(
            collective_id=2 if last else 1, has_side_effects=True
        ),
        cost_estimate=pl.CostEstimate(
            flops=10**10, bytes_accessed=10**8, transcendentals=0
        ),
        name="reduce_last" if last else "reduce_norm_gather",
    )(*operands)


def shards(
    tokens,
    sizes,
    ln1_gain,
    qkv_weight,
    proj_weight,
    ln2_gain,
    fc1_weight,
    fc1_bias,
    fc2_weight,
    pair_source,
    pair_target,
    kept_order,
):
    images, own_tokens, width = tokens.shape
    length = sizes.shape[1]
    kept_total = kept_order.shape[1]
    count = lax.axis_size("mp")
    me = lax.axis_index("mp")
    kept_own = kept_total // count
    padded = -(-kept_own // 16) * 16
    head_size = width // HEADS
    local_width = qkv_weight.shape[2]
    local_heads = local_width // head_size

    base = tokens.astype(jnp.float32)
    normed = layer_norm(base, ln1_gain).astype(jnp.bfloat16)
    whole, heads_whole = gather_all(
        normed.reshape(own_tokens, width),
        jnp.concatenate(
            [qkv_weight[0], qkv_weight[1], qkv_weight[2], proj_weight.T], axis=1
        ),
    )
    whole = whole[None]
    whole, heads_whole, late = lax.optimization_barrier((whole, heads_whole, fc1_weight))
    fc1 = lax.all_gather(late, "dp", axis=0, tiled=True)

    positions = jnp.arange(length, dtype=jnp.int32)
    order = jnp.pad(
        kept_order.reshape(images, count, kept_own),
        ((0, 0), (0, 0), (0, padded - kept_own)),
        constant_values=-1,
    ).reshape(images, count * padded)
    hits = positions[None, None, :] == pair_source[:, :, None]
    destination = positions[None, :] + jnp.sum(
        jnp.where(hits, pair_target[:, :, None] - positions[None, None, :], 0), axis=1
    )
    joins = order[:, :, None] == destination[:, None, :]
    shares = jnp.where(joins, sizes[:, None, :], 0.0)
    merged_size = jnp.sum(shares, axis=2, keepdims=True)
    shares = (shares / jnp.where(merged_size > 0, merged_size, 1.0)).astype(jnp.bfloat16)
    own_shares = lax.dynamic_slice_in_dim(shares, me * own_tokens, own_tokens, 2)

    projected = jnp.einsum(
        "ind,df->inf", whole, heads_whole[:, : 3 * local_width], preferred_element_type=jnp.float32
    ).astype(jnp.bfloat16)
    shaped = [
        projected[:, :, c * local_width : (c + 1) * local_width].reshape(
            images, length, local_heads, head_size
        )
        for c in range(3)
    ]
    size_bias = jnp.log(sizes)[:, None, None, :]
    block = min(512, length)
    outputs = []
    for begin in range(0, length, block):
        scores = (
            jnp.einsum(
                "iqhe,ikhe->ihqk",
                shaped[0][:, begin : begin + block],
                shaped[1],
                preferred_element_type=jnp.float32,
            )
            / math.sqrt(head_size)
            + size_bias
        )
        weights = jax.nn.softmax(scores, axis=-1).astype(jnp.bfloat16)
        outputs.append(
            jnp.einsum("ihqk,ikhe->iqhe", weights, shaped[2], preferred_element_type=jnp.float32)
            .astype(jnp.bfloat16)
            .reshape(images, block, local_width)
        )
    attended = jnp.concatenate(outputs, axis=1)

    joined = jnp.einsum(
        "ijn,ind->ijd", shares, attended, preferred_element_type=jnp.float32
    ).astype(jnp.bfloat16)

    left, right = lax.optimization_barrier(
        (
            jnp.concatenate([joined, own_shares], axis=2),
            jnp.concatenate([heads_whole[:, 3 * local_width :].T, tokens[0]], axis=0),
        )
    )
    parts = jnp.einsum("ijd,de->ije", left, right, preferred_element_type=jnp.float32)
    parts = parts.astype(jnp.bfloat16).reshape(count, padded, width)
    merged, gathered, fc2 = reduce_parts(parts, ln2_gain.reshape(1, width), fc2_weight.T)
    hidden_sum = jnp.einsum(
        "md,df->mf", gathered.reshape(count * padded, width), fc1,
        preferred_element_type=jnp.float32,
    )
    hidden = jax.nn.gelu(hidden_sum + fc1_bias).astype(jnp.bfloat16)
    partial_out = jnp.einsum("mf,df->md", hidden, fc2, preferred_element_type=jnp.float32)
    partial_out = partial_out.astype(jnp.bfloat16).reshape(count, padded, width)
    out = reduce_parts(partial_out, merged)[0]
    return out[None, :kept_own]


LOG2E = math.log2(math.e)
KINDS = ("E1", "E2", "Y4", "N1", "N2", "M1", "M2", "M3", "M4", "Y1", "Y2", "Y3")
E1, E2, Y4, N1, N2, M1, M2, M3, M4, Y1, Y2, Y3 = KINDS
S0 = "s0"
ARRAYS = ("kv0", "kv1", "q", "p", "f1a", "f1b", "f2a", "f2b", "f2c")
W_KV0, W_KV1, W_Q, W_P, W_F1A, W_F1B, W_F2A, W_F2B, W_F2C = ARRAYS
DOWN = (W_F2A, W_F2B, W_F2C)

SCHEDULE = {
    "go": (((S0, W_KV0), (S0, W_KV1), (S0, W_Q)), ((S0, W_KV0), (S0, W_KV1), (S0, W_Q))),
    "tb": (((M1, W_KV0), (Y1, W_KV0), (Y1, W_KV1), (M1, W_KV1), (S0, W_P), (M2, W_KV0), (Y1, W_Q), (M2, W_KV1), (S0, W_F1A)), ((N1, W_KV0), (E1, W_KV0), (E1, W_KV1), (N1, W_KV1), (E1, W_Q), (S0, W_P), (N2, W_KV0), (N2, W_KV1), (Y1, W_KV0), (Y1, W_Q), (N1, W_Q), (N2, W_Q), (E1, W_P), (S0, W_F1A))),
    "tk": (((M3, W_KV0), (M1, W_Q)), ((Y1, W_KV1),)),
    "w0": (((M3, W_KV1), (Y1, W_F1A), (M2, W_Q), (Y1, W_P), (M3, W_Q), (S0, W_F1B), (M1, W_F1A)), ()),
    "w1": (((M2, W_P), (M1, W_P)), ((N1, W_P), (N2, W_P), (Y1, W_P), (E1, W_F1A))),
    "sr": (((M3, W_P), (S0, W_F2A)), ((S0, W_F1B),)),
    "a0": ((), ((N2, W_F1A),)),
    "r0": (((Y1, W_F1B),), ()),
    "a4": (((M3, W_F1A),), ()),
    "a5": ((), ((N1, W_F1A),)),
    "a8": (((Y1, W_F2A), (M2, W_F1A), (S0, W_F2B)), ((N1, W_F1B), (S0, W_F2A))),
    "a10": ((), ((E1, W_F1B),)),
    "a12": (((M2, W_F1B),), ((Y1, W_F1A),)),
    "r3": ((), ((N1, W_F2A),)),
    "rr": (((S0, W_F2C), (M1, W_F1B), (M2, W_F2A), (M1, W_F2A)), ((E1, W_F2A), (N2, W_F1B), (S0, W_F2B), (N2, W_F2A))),
    "nm": (((Y1, W_F2B), (M3, W_F1B), (Y1, W_F2C), (M3, W_F2A)), ((Y1, W_F1B), (S0, W_F2C))),
    "e0": (((M1, W_F2C),), ((N1, W_F2B),)),
    "e1": (((M2, W_F2B),), ((E1, W_F2C), (N1, W_F2C), (E1, W_F2B), (N2, W_F2C))),
    "e2": (((M2, W_F2C),), ((N2, W_F2B), (Y1, W_F2C), (Y1, W_F2B))),
    "e3": (((M3, W_F2C),), ((Y1, W_F2A),)),
    "n0": (((M3, W_F2B),), ()),
    "n1": (((M1, W_F2B),), ()),
}


def nt_dot(left, right):
    return lax.dot_general(
        left, right, (((1,), (1,)), ((), ())), preferred_element_type=jnp.float32
    )


INNER, OUTER, PAIR = "inner", "outer", "pair"
START = (((E1, INNER), (Y1, PAIR)), ((M1, OUTER), (N1, INNER), (Y1, PAIR)))
RELAY = {
    (0, M1): ((Y4, 1, PAIR, 0),),
    (0, Y1): ((E2, PAIR, INNER, None),),
    (0, M2): ((Y2, 2, PAIR, None),),
    (0, M3): ((Y3, 3, PAIR, None),),
    (1, N1): ((M2, 1, OUTER, None), (Y2, 1, PAIR, None)),
    (1, E1): ((N2, OUTER, INNER, None),),
    (1, Y1): ((M4, PAIR, OUTER, 1),),
    (1, N2): ((M3, 2, OUTER, None), (Y3, 2, PAIR, None)),
}


class Streams:
    def __init__(self, dp, homes, send, recv, local):
        me = lax.axis_index("dp")
        z, y = lax.div(me, 2), lax.rem(me, 2)
        high = lax.div(z, 2)
        step = 1 - 2 * high
        self.end = lax.rem(lax.div(z + 1, 2), 2) == 0
        self.mid = lax.rem(lax.div(z + 1, 2), 2) == 1
        self.me = me
        self.pair = z * 2 + 1 - y
        self.inner = (z + step) * 2 + y
        self.outer = lax.rem((z - step) * 2 + y + dp, dp)
        middle = lax.rem(lax.div(z + 1, 2), 2)
        self.turns = [
            z + step * (a + middle * (b - a)) for a, b in ((0, 0), (2, -1), (3, 1), (1, 2))
        ]
        self.ahead = [lax.rem((z + step * k) * 2 + y + dp, dp) for k in range(4)]
        self.homes, self.send, self.recv, self.local = homes, send, recv, local
        self.peers = {INNER: self.inner, OUTER: self.outer, PAIR: self.pair}

    def block(self, name, owner, part=None):
        _, target, stride, low, count = self.homes[name]
        if part is not None:
            first = -(-count // 32) * 16
            low, count = low + part * first, (first, count - first)[part]
        return target(pl.ds(pl.multiple_of(owner * stride + low, 16), count))

    def own(self, name):
        return self.homes[name][0]

    def copy(self, name, kind, source, target, peer):
        number = ARRAYS.index(name) * len(KINDS) + KINDS.index(kind)
        return pltpu.make_async_remote_copy(
            src_ref=source,
            dst_ref=target,
            send_sem=self.send.at[number],
            recv_sem=self.recv.at[number],
            device_id={"dp": self.peers[peer]},
            device_id_type=pl.DeviceIdType.MESH,
        )

    def move(self, name, kind, owner, peer, part=None):
        block = self.block(name, owner, part)
        self.copy(name, kind, block, block, peer).start()

    def arrived(self, name, *kinds):
        for kind in kinds:
            block = self.block(name, self.me, {"Y4": 0, "M4": 1}.get(kind))
            self.copy(name, kind, block, block, "pair").wait_recv()

    def stay(self, name):
        return pltpu.make_async_copy(
            self.own(name), self.block(name, self.me), self.local.at[ARRAYS.index(name)]
        )

    def act(self, role, what, name):
        if what == S0:
            here = self.block(name, self.me)
            for kind, peer in START[role]:
                own = here if self.own(name) is None else self.own(name)
                self.copy(name, kind, own, here, peer).start()
            if self.own(name) is not None:
                self.stay(name).start()
            return
        self.arrived(name, what)
        for kind, owner, peer, part in RELAY[role, what]:
            who = {PAIR: self.pair, OUTER: self.outer}.get(owner)
            self.move(name, kind, self.ahead[owner] if who is None else who, peer, part)

    def serve(self, point, when=None):
        for role, here in ((0, self.end), (1, self.mid)):
            todo = SCHEDULE.get(point, ((), ()))[role]
            if todo:
                condition = here if when is None else jnp.logical_and(when, here)

                @pl.when(condition)
                def _():
                    for what, name in todo:
                        self.act(role, what, name)

    def near(self, name):
        if self.own(name) is not None:
            self.stay(name).wait()

        @pl.when(self.end)
        def _():
            self.arrived(name, "M4", "Y4")

        @pl.when(self.mid)
        def _():
            self.arrived(name, "E2")

    def pair_ready(self, name, turn):
        if turn == 0:
            if self.own(name) is not None:
                self.stay(name).wait()
            return

        @pl.when(self.end)
        def _():
            self.arrived(name, *(("Y2",), ("Y3",), ("Y4", "M4"))[turn - 1])

        @pl.when(self.mid)
        def _():
            self.arrived(name, *(("E2",), ("Y2",), ("Y3",))[turn - 1])

    def full(self, name):
        self.near(name)
        self.arrived(name, "Y2", "Y3")

    def sent(self, name):
        def drain(*kinds):
            for kind in kinds:
                block = self.block(name, self.me, {"Y4": 0, "M4": 1}.get(kind))
                self.copy(name, kind, block, block, "pair").wait_send()

        drain("Y1", "Y2", "Y3")

        @pl.when(self.end)
        def _():
            drain("E1", "E2", "Y4")

        @pl.when(self.mid)
        def _():
            drain("N1", "N2", "M1", "M2", "M3", "M4")


def column_of(row, count):
    down = lax.broadcasted_iota(jnp.int32, (count, count), 0)
    over = lax.broadcasted_iota(jnp.int32, (count, count), 1)
    return jnp.sum(jnp.where(down == over, row, 0.0), axis=1, keepdims=True)


def layer_kernel(dp, mp, kept_own, *refs):
    (tokens, sizes, gain_one, qkv, proj, gain_two, fc1, bias, fc2, source, target, order) = refs[:12]
    out = refs[12]
    (tok, raw_qkv, raw_proj, whole, wkv, packed_q, packed_p, wq, wp, w1, w2, shares, picks, own_share, source_share,
     kbuf, vbuf, qall, qbuf, source_att, attb, joined, parts, landing, merged, again, hidden,
     merged_out, ready_out, landing_out, own_out, done_out,
     send, recv, local, msend, mrecv) = refs[13:]
    rows, width = tok.shape
    length = sizes.shape[1]
    local_width = joined.shape[1]
    local_heads, _, lanes = kbuf.shape
    head_size = local_width // local_heads
    at = lax.axis_index("mp")
    block_of = [toggled(at, k) for k in range(mp)]
    pair, across = block_of[1], block_of[2]

    cut = fc1.shape[1] // 2
    shard = fc1.shape[0]
    homes = {
        "kv0": (None, lambda r: wkv.at[r, :], shard, 0, shard // 2),
        "kv1": (None, lambda r: wkv.at[r, :], shard, shard // 2, shard // 2),
        "q": (None, lambda r: packed_q.at[r, :], shard // 2, 0, shard // 2),
        "p": (None, lambda r: packed_p.at[r, :], shard // 2, 0, shard // 2),
        "f1a": (fc1.at[:, pl.ds(0, cut)], lambda r: w1.at[r, pl.ds(0, cut)], shard, 0, shard),
        "f1b": (fc1.at[:, pl.ds(cut, cut)], lambda r: w1.at[r, pl.ds(cut, cut)], shard, 0, shard),
        "f2a": (fc2.at[:, pl.ds(0, cut)], lambda r: w2.at[r, pl.ds(0, cut)], shard, 0, shard),
        "f2b": (
            fc2.at[pl.ds(0, shard // 2), pl.ds(cut, cut)],
            lambda r: w2.at[r, pl.ds(cut, cut)], shard, 0, shard // 2,
        ),
        "f2c": (
            fc2.at[pl.ds(shard // 2, shard // 2), pl.ds(cut, cut)],
            lambda r: w2.at[r, pl.ds(cut, cut)], shard, shard // 2, shard // 2,
        ),
    }
    st = Streams(dp, homes, send, recv, local)

    load = pltpu.make_async_copy(tokens, tok, local.at[len(ARRAYS)])
    load.start()
    load_qkv = pltpu.make_async_copy(qkv, raw_qkv, local.at[len(ARRAYS) + 1])
    load_qkv.start()
    load_proj = pltpu.make_async_copy(proj, raw_proj, local.at[len(ARRAYS) + 2])
    load_proj.start()

    barrier = pltpu.get_barrier_semaphore()

    def hello(axis, peer):
        pl.semaphore_signal(
            barrier, inc=1, device_id={axis: peer}, device_id_type=pl.DeviceIdType.MESH
        )

    hello("dp", st.pair)
    hello("dp", st.inner)
    hello("mp", pair)
    hello("mp", across)

    @pl.when(st.mid)
    def _():
        hello("dp", st.outer)

    load_qkv.wait()
    load_proj.wait()
    mine = pl.ds(pl.multiple_of(st.me * shard, shard), shard)
    wkv[mine, 0:local_width] = raw_qkv[1]
    wkv[mine, local_width : 2 * local_width] = raw_qkv[2]
    few = shard // 2
    mine = pl.ds(pl.multiple_of(st.me * few, few), few)
    for packed, raw in ((packed_q, raw_qkv.at[0]), (packed_p, raw_proj)):
        packed[mine, 0:local_width] = raw[0:few]
        packed[mine, local_width : 2 * local_width] = raw[few:shard]

    def unpack(packed, flat):
        def one(owner, carry):
            there = pl.ds(pl.multiple_of(owner * few, few), few)
            for side in range(2):
                here = pl.ds(pl.multiple_of(owner * shard + side * few, few), few)
                flat[here, :] = packed[there, side * local_width : (side + 1) * local_width]
            return carry

        lax.fori_loop(0, dp, one, 0)

    @pl.when(st.end)
    def _():
        pl.semaphore_wait(barrier, 4)

    @pl.when(st.mid)
    def _():
        pl.semaphore_wait(barrier, 5)

    st.serve("go")

    made = []

    def give(src, dst, peer):
        copy = pltpu.make_async_remote_copy(
            src_ref=src,
            dst_ref=dst,
            send_sem=msend.at[len(made)],
            recv_sem=mrecv.at[len(made)],
            device_id={"mp": peer},
            device_id_type=pl.DeviceIdType.MESH,
        )
        copy.start()
        made.append(copy)
        return copy

    load.wait()
    slab = 32
    first_gain = gain_one[...].reshape(1, width)
    second_gain = gain_two[...].reshape(1, width)
    first_bias = bias[...].reshape(1, bias.shape[0])

    def norm_rows(i, carry):
        span = pl.ds(pl.multiple_of(i * slab, slab), slab)
        whole[at, span, :] = layer_norm(
            tok[span, :].astype(jnp.float32), first_gain
        ).astype(jnp.bfloat16)
        return carry

    lax.fori_loop(0, rows // slab, norm_rows, 0)
    token_pair = give(whole.at[at], whole.at[at], pair)
    token_across = give(whole.at[at], whole.at[at], across)
    st.serve("ln")

    position = lax.broadcasted_iota(jnp.int32, (1, length), 1).astype(jnp.float32)
    count = source.shape[1]
    source_column = column_of(source[...].astype(jnp.float32), count)
    target_column = column_of(target[...].astype(jnp.float32), count)
    destination = position + jnp.sum(
        jnp.where(position == source_column, target_column - position, 0.0),
        axis=0,
        keepdims=True,
    )
    size_row = sizes[...]
    order_row = order[...].astype(jnp.float32)

    picked = (position == source_column).astype(jnp.bfloat16)

    def table(b, carry):
        shape = (rows, order.shape[1])
        down = lax.broadcasted_iota(jnp.int32, shape, 0)
        over = lax.broadcasted_iota(jnp.int32, shape, 1)
        mine = jnp.logical_and(over == down + b * kept_own, down < kept_own)
        wanted = jnp.sum(jnp.where(mine, order_row + 1.0, 0.0), axis=1, keepdims=True) - 1.0
        share = jnp.where(wanted == destination, size_row, 0.0)
        total = jnp.sum(share, axis=1, keepdims=True)
        share = share / jnp.where(total > 0, total, 1.0)
        shares[b] = share.astype(jnp.bfloat16)
        here = wanted == position
        picks[b] = jnp.where(here, 1.0, 0.0).astype(jnp.bfloat16)
        own_share[b] = jnp.sum(jnp.where(here, share, 0.0), axis=1, keepdims=True)
        source_share[b] = nt_dot(share.astype(jnp.bfloat16), picked).astype(jnp.bfloat16)
        return carry

    lax.fori_loop(0, mp, table, 0)
    lane = lax.broadcasted_iota(jnp.int32, (length, lanes), 1)
    for h in range(local_heads):
        kbuf[h] = jnp.zeros((length, lanes), jnp.bfloat16)
        qbuf[h] = jnp.zeros((rows, lanes), jnp.bfloat16)
        vbuf[h] = jnp.where(lane == head_size, 1.0, 0.0).astype(jnp.bfloat16)
    size_bias = jnp.log(size_row) * LOG2E

    st.serve("tb")
    token_across.wait_recv()
    token_far = give(whole.at[across], whole.at[across], pair)
    st.serve("tk")
    token_pair.wait_recv()
    token_far.wait_recv()

    def project_kv(b, carry):
        product = jnp.dot(whole[b], wkv[...], preferred_element_type=jnp.float32)
        product = product.astype(jnp.bfloat16)
        span = pl.ds(pl.multiple_of(b * rows, rows), rows)
        for h in range(local_heads):
            low = h * head_size
            kbuf[h, span, 0:head_size] = product[:, low : low + head_size]
            low = low + local_width
            vbuf[h, span, 0:head_size] = product[:, low : low + head_size]
        return carry

    factor = LOG2E / math.sqrt(head_size)

    def project_q(b, carry):
        product = jnp.dot(whole[b], wq[...], preferred_element_type=jnp.float32)
        span = pl.ds(pl.multiple_of(b * rows, rows), rows)
        qall[span, :] = (product * factor).astype(jnp.bfloat16)
        return carry

    st.serve("w0")
    st.full("kv0")
    st.full("kv1")
    lax.fori_loop(0, mp, project_kv, 0)
    st.serve("w1")
    st.full("q")
    unpack(packed_q, wq)
    lax.fori_loop(0, mp, project_q, 0)

    def heads_of(product):
        chosen = product.astype(jnp.bfloat16)
        for h in range(local_heads):
            low = h * head_size
            yield h, chosen[:, low : low + head_size]

    def mix(query, h):
        scores = nt_dot(query, kbuf[h]) + size_bias
        top = jnp.max(scores, axis=1, keepdims=True)
        weights = jnp.exp2(scores - top).astype(jnp.bfloat16)
        mixed = jnp.dot(weights, vbuf[h], preferred_element_type=jnp.float32)
        return mixed / mixed[:, head_size : head_size + 1]

    st.serve("sr")
    product = jnp.dot(picked, qall[...], preferred_element_type=jnp.float32)
    for h, query in heads_of(product):
        qbuf[h, 0:count, 0:head_size] = query

    def attend_source(h, carry):
        source_att[h] = mix(qbuf[h, 0:count, :], h).astype(jnp.bfloat16)
        return carry

    lax.fori_loop(0, local_heads, attend_source, 0)

    def part_of(turn, block):
        product = jnp.dot(picks[block], qall[...], preferred_element_type=jnp.float32)
        for h, query in heads_of(product):
            qbuf[h, :, 0:head_size] = query

        def attend(h, carry):
            for n in range(local_heads):
                st.serve(f"a{turn * local_heads + n}", h == n)
            taken = jnp.dot(
                source_share[block], source_att[h], preferred_element_type=jnp.float32
            )
            attb[h] = (mix(qbuf[h], h) * own_share[block] + taken).astype(jnp.bfloat16)
            return carry

        lax.fori_loop(0, local_heads, attend, 0)
        for h in range(local_heads):
            joined[:, h * head_size : (h + 1) * head_size] = attb[h, :, 0:head_size]
        st.serve(f"r{turn}")
        if turn == 0:
            st.full("p")
            unpack(packed_p, wp)
        kept = shares[block, :, pl.ds(pl.multiple_of(at * rows, rows), rows)]
        return nt_dot(joined[...], wp[...]) + jnp.dot(
            kept, tok[...], preferred_element_type=jnp.float32
        )

    parts[2] = part_of(0, block_of[3]).astype(jnp.bfloat16)
    first = give(parts.at[2], landing.at[2], pair)
    total = part_of(1, across)
    first.wait_recv()
    parts[1] = (total + landing[2].astype(jnp.float32)).astype(jnp.bfloat16)
    second = give(parts.at[1], landing.at[1], across)
    parts[0] = part_of(2, pair).astype(jnp.bfloat16)
    third = give(parts.at[0], landing.at[0], pair)
    merged[...] = part_of(3, at)
    st.serve("rr")
    third.wait_recv()
    second.wait_recv()

    def norm_again(i, carry):
        span = pl.ds(pl.multiple_of(i * slab, slab), slab)
        total = (
            merged[span, :]
            + landing[0, span, :].astype(jnp.float32)
            + landing[1, span, :].astype(jnp.float32)
        )
        merged[span, :] = total
        again[at, span, :] = layer_norm(total, second_gain).astype(jnp.bfloat16)
        return carry

    lax.fori_loop(0, rows // slab, norm_again, 0)
    norm_pair = give(again.at[at], again.at[at], pair)
    norm_across = give(again.at[at], again.at[at], across)
    for column in range(4):
        merged_out[column] = merged[:, column * 2 * shard : (column + 1) * 2 * shard]
    st.serve("nm")
    st.full("f1a")
    st.full("f1b")

    def expand(block):
        product = jnp.dot(again[block], w1[...], preferred_element_type=jnp.float32)
        hidden[block] = jax.nn.gelu(product + first_bias).astype(jnp.bfloat16)

    expand(at)
    st.serve("e0")
    norm_pair.wait_recv()
    expand(pair)
    st.serve("e1")
    norm_across.wait_recv()
    norm_far = give(again.at[across], again.at[across], pair)
    st.serve("ag")
    expand(across)
    st.serve("e2")
    norm_far.wait_recv()
    expand(block_of[3])
    st.serve("e3")

    quarter = 2 * shard

    def fold(values):
        return jnp.concatenate([values[: rows // 2], values[rows // 2 :]], axis=1)

    def unfold(values):
        return jnp.concatenate([values[:, :quarter], values[:, quarter:]], axis=0)

    flights = []
    for turn in range(4):
        for name in DOWN:
            st.pair_ready(name, turn)
        columns = pl.ds(pl.multiple_of(st.turns[turn] * quarter, quarter), quarter)
        ready, landed = ready_out.at[turn], landing_out.at[turn]

        def piece(block):
            return nt_dot(hidden[block], w2[columns, :])

        ready[2] = fold(piece(block_of[3])).astype(jnp.bfloat16)
        one = give(ready.at[2], landed.at[2], pair)
        ready[0] = fold(piece(pair)).astype(jnp.bfloat16)
        three = give(ready.at[0], landed.at[0], pair)
        total = fold(piece(across))
        one.wait_recv()
        ready[1] = (total + landed[2].astype(jnp.float32)).astype(jnp.bfloat16)
        two = give(ready.at[1], landed.at[1], across)
        own_out[turn] = merged_out[st.turns[turn]] + piece(at)
        st.serve(f"n{turn}")
        flights.append((three, two))
    for turn, flight in enumerate(flights):
        for copy in flight:
            copy.wait_recv()
        landed = landing_out[turn, 0].astype(jnp.float32) + landing_out[turn, 1].astype(
            jnp.float32
        )
        done_out[st.turns[turn]] = (own_out[turn] + unfold(landed)).astype(jnp.bfloat16)
    for column in range(4):
        out[:, column * quarter : (column + 1) * quarter] = done_out[column]
    for name in ARRAYS:
        st.sent(name)
    for copy in made:
        copy.wait_send()


def whole_layer(tokens, sizes, ln1_gain, qkv_weight, proj_weight, ln2_gain, fc1_weight, fc1_bias,
                fc2_weight, pair_source, pair_target, kept_order):
    dp, mp = lax.axis_size("dp"), lax.axis_size("mp")
    _, rows, width = tokens.shape
    length = sizes.shape[1]
    kept_own = kept_order.shape[1] // mp
    local_width = qkv_weight.shape[2]
    local_heads = HEADS * local_width // width
    head_size = local_width // local_heads
    lanes = -(-(head_size + 1) // 128) * 128
    hidden = fc1_weight.shape[1]
    bf16, f32 = jnp.bfloat16, jnp.float32
    vmem = pl.BlockSpec(memory_space=pltpu.VMEM)
    hbm = pl.BlockSpec(memory_space=pl.ANY)
    shard, count = fc1_weight.shape[0], pair_source.shape[1]
    scratch = [
        pltpu.VMEM((rows, width), bf16),
        pltpu.VMEM((3, shard, local_width), bf16),
        pltpu.VMEM((shard, local_width), bf16),
        pltpu.VMEM((mp, rows, width), bf16),
        pltpu.VMEM((width, 2 * local_width), bf16),
        pltpu.VMEM((width // 2, 2 * local_width), bf16),
        pltpu.VMEM((width // 2, 2 * local_width), bf16),
        pltpu.VMEM((width, local_width), bf16),
        pltpu.VMEM((width, local_width), bf16),
        pltpu.VMEM((width, hidden), bf16),
        pltpu.VMEM((width, hidden), bf16),
        pltpu.VMEM((mp, rows, length), bf16),
        pltpu.VMEM((mp, rows, length), bf16),
        pltpu.VMEM((mp, rows, 1), f32),
        pltpu.VMEM((mp, rows, count), bf16),
        pltpu.VMEM((local_heads, length, lanes), bf16),
        pltpu.VMEM((local_heads, length, lanes), bf16),
        pltpu.VMEM((length, local_width), bf16),
        pltpu.VMEM((local_heads, rows, lanes), bf16),
        pltpu.VMEM((local_heads, count, lanes), bf16),
        pltpu.VMEM((local_heads, rows, lanes), bf16),
        pltpu.VMEM((rows, local_width), bf16),
        pltpu.VMEM((mp - 1, rows, width), bf16),
        pltpu.VMEM((mp - 1, rows, width), bf16),
        pltpu.VMEM((rows, width), f32),
        pltpu.VMEM((mp, rows, width), bf16),
        pltpu.VMEM((mp, rows, hidden), bf16),
        pltpu.VMEM((4, rows, 2 * shard), f32),
        pltpu.VMEM((4, mp - 1, rows // 2, 4 * shard), bf16),
        pltpu.VMEM((4, mp - 1, rows // 2, 4 * shard), bf16),
        pltpu.VMEM((4, rows, 2 * shard), f32),
        pltpu.VMEM((4, rows, 2 * shard), bf16),
        pltpu.SemaphoreType.DMA((len(ARRAYS) * len(KINDS),)),
        pltpu.SemaphoreType.DMA((len(ARRAYS) * len(KINDS),)),
        pltpu.SemaphoreType.DMA((len(ARRAYS) + 3,)),
        pltpu.SemaphoreType.DMA((24,)),
        pltpu.SemaphoreType.DMA((24,)),
    ]
    out = pl.pallas_call(
        functools.partial(layer_kernel, dp, mp, kept_own),
        out_shape=jax.ShapeDtypeStruct((rows, width), bf16),
        in_specs=[hbm, vmem, vmem, hbm, hbm, vmem, hbm, vmem, hbm, vmem, vmem, vmem],
        out_specs=vmem,
        scratch_shapes=scratch,
        compiler_params=pltpu.CompilerParams(
            collective_id=3, has_side_effects=True, vmem_limit_bytes=60 * 2**20
        ),
        cost_estimate=pl.CostEstimate(flops=10**10, bytes_accessed=10**8, transcendentals=0),
        name="layer",
    )(
        tokens.reshape(rows, width),
        sizes,
        ln1_gain,
        qkv_weight,
        proj_weight.T,
        ln2_gain,
        fc1_weight,
        fc1_bias,
        fc2_weight.T,
        pair_source,
        pair_target,
        kept_order,
    )
    return out[None, :kept_own]


def solution(mesh):
    line_by_two = mesh.shape["dp"] == 8 and mesh.shape["mp"] == 4
    return jax.shard_map(
        whole_layer if line_by_two else shards,
        mesh=mesh,
        in_specs=(
            P("dp", "mp", None),
            P("dp", None),
            P(),
            P(None, "dp", "mp"),
            P("mp", "dp"),
            P(),
            P("dp", "mp"),
            P("mp"),
            P("mp", "dp"),
            P("dp", None),
            P("dp", None),
            P("dp", None),
        ),
        out_specs=P("dp", "mp", None),
        check_vma=False,
    )
```
